256 devices in a mesh: tower: 8 (over x, z_hi), px: 4 (over y), py: 8 (over z_lo, core).
Axes of the slice: x: 4, y: 4, z: 8 (z_hi: 2, z_lo: 4; z = z_hi * 4 + z_lo), core: 2. Of those that a mesh axis runs over, the one named last changes fastest.
Arguments:
- positions: float32 [3, 16, 8, 16, 128], P(None, 'tower', 'px', 'py'), may hold values from 0 to 1
- velocities: float32 [3, 16, 8, 16, 128], P(None, 'tower', 'px', 'py'), may hold values from -6 to 6
- types: int32 [16, 8, 16, 128], P('tower', 'px', 'py'), may hold values from 0 to 15
- strength: float32 [16], replicated, may hold values from 0.5 to 2
- counts: int32 [16, 8, 16], P('tower', 'px', 'py'), may hold values from 64 to 128
- pair_list: int32 [27, 16, 8, 16], P(None, 'tower', 'px', 'py'), may hold values from 0 to 1, as said below
- destination: int32 [16, 8, 16], P('tower', 'px', 'py'), may hold values from 0 to 3839, as said below
Outputs:
- moved_positions: float32 [3, 3840, 128], P(None, ('tower', 'px', 'py'))
- moved_velocities: float32 [3, 3840, 128], P(None, ('tower', 'px', 'py'))
The draws below stay inside these ranges and needn't reach their ends.
Inputs may be any that keep to these rules, and one draw needn't show every extreme that they name: pair_list[k] at cell c equals pair_list[26 - k] at the cell c plus the offset of k. `destination`: the values are distinct; a block's slot lies among the 15 slots (slot // 15 names a device, numbered tower-major, then px, then py) of a device with the same tower index and the same px index as the block's owner; from each device either no block or exactly 2 blocks go to other devices, at most 1 of them to any one device; among the devices of one tower index and one px index, one device receives exactly 1 block from every other and holds exactly 15 blocks afterwards.
All inputs are finite; a program needn't handle non-finite values.
Results may differ from the reference program's by a relative error of at most 0.0001.
Values sent between devices are 32-bit elements; how exact they have to be, the bound alone decides.
A program may use at most 64 MiB of HBM per device.

```python
import math
import jax
import jax.numpy as jnp
from jax import lax

CZ = 2
CX = 2
CY = 2
A = 128
NT = 16
STEPS = 4
GZ = 16
GX = 8
GY = 16
SLOTS = 3840
N_TOWER = 8
N_PX = 4
N_PY = 8


def draw_pair_list(key, part):
    grid_z = CZ * N_TOWER
    grid_x = CX * N_PX
    grid_y = CY * N_PY
    halves = (jax.random.randint(jax.random.fold_in(key, 101), (13, grid_z, grid_x, grid_y), 0, 5) > 0).astype(jnp.int32)
    selfs = (jax.random.randint(jax.random.fold_in(key, 102), (grid_z, grid_x, grid_y), 0, 5) > 0).astype(jnp.int32)
    flags = [selfs] * 27
    counter = 0
    for offset_id in range(27):
        first = offset_id // 9 - 1
        second = offset_id // 3 % 3 - 1
        third = offset_id % 3 - 1
        forward = second == 1 or (second == 0 and third == 1) or (second == 0 and third == 0 and (first == 1))
        if forward:
            flags[offset_id] = halves[counter]
            flags[26 - offset_id] = jnp.roll(halves[counter], (first, second, third), axis=(0, 1, 2))
            counter = counter + 1
    flags[13] = selfs
    return jnp.stack(flags)


def group_destination(group_key, group_id):
    plane = N_PY
    blocks = CZ * CX * CY
    move = blocks // 4
    peer = max(blocks // 8, 1)
    cap = blocks + (plane - 1) * peer
    hot = jax.random.randint(jax.random.fold_in(group_key, 1), (), 0, plane)
    device = jnp.arange(plane, dtype=jnp.int32)[:, None]
    keys = jax.random.split(jax.random.fold_in(group_key, 2), plane)
    perms = jax.vmap(lambda k: jax.random.permutation(k, blocks))(keys)
    rank = jnp.argsort(perms, axis=1).astype(jnp.int32)
    cycle = (device - hot - 1) % plane
    mover = (rank < move) & (device != hot)
    group = rank // peer
    other = (hot + 1 + (cycle + group) % (plane - 1)) % plane
    goal = jnp.where(mover, jnp.where(group == 0, hot, other), device).astype(jnp.int32)
    flat_goal = goal.reshape(plane * blocks)
    order = jax.random.permutation(jax.random.fold_in(group_key, 3), plane * blocks)
    sorted_goal = flat_goal[order]
    onehot = (sorted_goal[:, None] == jnp.arange(plane, dtype=jnp.int32)[None, :]).astype(jnp.int32)
    seat_sorted = jnp.sum(jnp.cumsum(onehot, axis=0) * onehot, axis=1) - 1
    seat = jnp.zeros((plane * blocks,), jnp.int32).at[order].set(seat_sorted)
    value = (group_id * plane + flat_goal) * cap + seat
    grid = value.reshape(N_PY, CZ, CX, CY).transpose(1, 2, 0, 3)
    return grid.reshape(CZ, CX, CY * N_PY)


def draw_destination(key, part):
    slabs = []
    for tower_id in range(N_TOWER):
        rows = []
        for plate_id in range(N_PX):
            group_id = tower_id * N_PX + plate_id
            rows.append(group_destination(jax.random.fold_in(key, 200 + group_id), group_id))
        slabs.append(jnp.concatenate(rows, axis=1))
    return jnp.concatenate(slabs, axis=0).astype(jnp.int32)


def with_ends(entries, key, least, high):
    shape = entries.shape
    index_at = [jax.random.randint(jax.random.fold_in(key, axis), (), 0, shape[axis]) for axis in range(len(shape))]
    entries = entries.at[tuple(index_at)].set(least)
    longest = shape.index(max(shape))
    index_at[longest] = (index_at[longest] + 1) % shape[longest]
    return entries.at[tuple(index_at)].set(high)


def block_scale(rng, dims, cuts, low, largest):
    gain = 1.0
    for axis_at, parts in cuts:
        steps = jax.random.uniform(jax.random.fold_in(jax.random.fold_in(rng, 6), axis_at), (parts,), jnp.float32, low / len(cuts), largest / len(cuts))
        gain = gain * jnp.repeat(jnp.exp(steps), dims[axis_at] // parts).reshape((-1,) + (1,) * (len(dims) - 1 - axis_at))
    return gain


def scatter_about(own_key, extent, width, bound, cuts=(), kind=jnp.bfloat16):
    gain = block_scale(own_key, extent, cuts, -0.22, 0.18) if cuts else 1.0
    entries = jax.random.normal(own_key, extent, jnp.float32) * width * gain
    return jnp.minimum(jnp.maximum(entries, -bound), bound).astype(kind)


def setup_inputs(seed: int = 0) -> dict:
    arg_keys = jax.random.split(jax.random.key(seed), 8)
    positions = jnp.clip(1.0 * jax.random.uniform(arg_keys[0], (3, GZ, GX, GY, A), jnp.float32) ** block_scale(arg_keys[0], (3, GZ, GX, GY, A), ((1, 8), (2, 4), (3, 8)), -0.2, 0.2), 0.0, 1.0)
    velocities = scatter_about(arg_keys[1], (3, GZ, GX, GY, A), 1.0, 6.0, ((1, 8), (2, 4), (3, 8)), jnp.float32)
    types = with_ends(jax.random.randint(arg_keys[2], (GZ, GX, GY, A), 0, NT), jax.random.fold_in(arg_keys[2], 1), 0, NT - 1).astype(jnp.int32)
    strength = jnp.clip(jnp.exp(jax.random.uniform(arg_keys[3], (NT,), jnp.float32, math.log(0.5), math.log(2.0))), 0.5, 2.0)
    counts = with_ends(jax.random.randint(arg_keys[4], (GZ, GX, GY), A // 2, A + 1), jax.random.fold_in(arg_keys[4], 1), A // 2, A).astype(jnp.int32)
    pair_list = draw_pair_list(jax.random.fold_in(arg_keys[7], 71), 0)
    destination = draw_destination(jax.random.fold_in(arg_keys[7], 71), 0)
    return dict(positions=positions, velocities=velocities, types=types, strength=strength, counts=counts, pair_list=pair_list, destination=destination)


step_time = 0.02


def offsets_of(offset_id):
    return offset_id // 9 - 1, offset_id // 3 % 3 - 1, offset_id % 3 - 1


def pair_terms(own, own_str, far, far_str, flag, offset):
    vec_shape = (3,) + (1,) * own.ndim
    offset_vec = jnp.array(offset, jnp.float32).reshape(vec_shape)
    delta = far[..., None, :] + offset_vec - own[..., :, None]
    square = jnp.sum(delta * delta, axis=0)
    weight = own_str[..., :, None] * far_str[..., None, :] * flag[..., None, None]
    factor = -6.0 * weight * jnp.square(jnp.maximum(1.0 - square, 0.0))
    return factor, delta


def total_force(positions, strength_atom, flags):
    grid_z, grid_x, grid_y, atoms = strength_atom.shape
    own_rows = jnp.moveaxis(positions, 1, 0).reshape(grid_z, 3, grid_x * grid_y, atoms)
    own_str = strength_atom.reshape(grid_z, grid_x * grid_y, atoms)
    force = jnp.zeros_like(own_rows)
    for offset_id in range(27):
        first, second, third = offsets_of(offset_id)
        far_pos = jnp.roll(positions, (-first, -second, -third), axis=(1, 2, 3))
        far_str = jnp.roll(strength_atom, (-first, -second, -third), axis=(0, 1, 2))
        far_rows = jnp.moveaxis(far_pos, 1, 0).reshape(grid_z, 3, grid_x * grid_y, atoms)
        far_str = far_str.reshape(grid_z, grid_x * grid_y, atoms)
        flag = flags[offset_id].reshape(grid_z, grid_x * grid_y)

        def slab_force(slab_item):
            own_p, own_s, far_p, far_s, flag_s = slab_item
            factor, delta = pair_terms(own_p, own_s, far_p, far_s, flag_s, (first, second, third))
            return jnp.sum(factor * delta, axis=-1)

        force = force + lax.map(slab_force, (own_rows, own_str, far_rows, far_str, flag))
    return jnp.moveaxis(force.reshape(grid_z, 3, grid_x, grid_y, atoms), 0, 1)


def reference(positions, velocities, types, strength, counts, pair_list, destination):
    kinds = strength.shape[0]
    slot_ids = lax.broadcasted_iota(jnp.int32, types.shape, 3)
    live = (slot_ids < counts[..., None]).astype(jnp.float32)
    kind_ids = lax.broadcasted_iota(jnp.int32, (kinds,) + types.shape, 0)
    table = strength.reshape((kinds, 1, 1, 1, 1))
    strength_atom = live * jnp.sum(jnp.where(types[None] == kind_ids, table, 0.0), axis=0)
    flags = pair_list.astype(jnp.float32)
    for step_id in range(STEPS):
        force = total_force(positions, strength_atom, flags)
        velocities = velocities + step_time * force
        positions = positions + step_time * velocities
    cells = live.shape[0] * live.shape[1] * live.shape[2]
    atoms = live.shape[3]
    flat_live = live.reshape(1, cells, atoms)
    flat_dest = destination.reshape(cells).astype(jnp.int32)
    moved_positions = jnp.zeros((3, SLOTS, atoms), jnp.float32).at[:, flat_dest].set(positions.reshape(3, cells, atoms) * flat_live)
    moved_velocities = jnp.zeros((3, SLOTS, atoms), jnp.float32).at[:, flat_dest].set(velocities.reshape(3, cells, atoms) * flat_live)
    return moved_positions, moved_velocities
```

```python
import itertools

import jax
import jax.numpy as jnp
from jax import lax
from jax.experimental import pallas as pl
from jax.experimental.pallas import tpu as pltpu
from jax.sharding import PartitionSpec as P

STEPS = 4
STEP_TIME = 0.02
KINDS = 16
SEATS = 15
ATOMS = 128
DEPTH = 192
MESH = pl.DeviceIdType.MESH
F32 = jnp.float32
BF16 = jnp.bfloat16

DIRECTIONS = sorted(
    (d for d in itertools.product((-1, 0, 1), repeat=3) if d != (0, 0, 0)),
    key=lambda d: abs(d[0]),
)
NEAR = 8
SEAT_OF_Y = {0: 0, 1: 1, -1: 2, 2: 3}


def spans(step):
    if step == 0:
        return pl.ds(1, 2), pl.ds(1, 2)
    return (pl.ds(2, 1), pl.ds(0, 1)) if step == 1 else (pl.ds(1, 1), pl.ds(3, 1))


def spans_y(step):
    if step == 0:
        return pl.ds(0, 2), pl.ds(0, 2)
    return (pl.ds(1, 1), pl.ds(2, 1)) if step == 1 else (pl.ds(0, 1), pl.ds(3, 1))


def thirds(x):
    high = x.astype(BF16).astype(F32)
    rest = x - high
    mid = rest.astype(BF16).astype(F32)
    return high, mid, rest - mid


def swap_halves(x):
    return jnp.concatenate([x[4:], x[:4]], axis=0)


def body(
    pos_ref, vel_ref, types_ref, strength_ref, counts_ref, pair_ref, dest_ref,
    out_pos_ref, out_vel_ref,
    region, speed, live_ref, flag_ref, left_ref, right_ref, value_ref, total, box, send_box,
    send_sem, recv_sem, move_send_sem, move_recv_sem,
):
    me_z, me_x, me_y = (lax.axis_index(a) for a in ("tower", "px", "py"))
    n_z, n_x, n_y = (lax.axis_size(a) for a in ("tower", "px", "py"))

    def device(d):
        return (
            lax.rem(me_z + d[0] + n_z, n_z),
            lax.rem(me_x + d[1] + n_x, n_x),
            lax.rem(me_y + d[2] + n_y, n_y),
        )

    peers = [(0, 0, r) for r in range(1, 8)]
    greeted = DIRECTIONS + [p for p in peers if p[2] not in (1, 7)]
    barrier = pltpu.get_barrier_semaphore()
    for d in greeted:
        pl.semaphore_signal(barrier, inc=1, device_id=device(d), device_id_type=MESH)

    row8 = lax.broadcasted_iota(jnp.int32, (8, ATOMS), 0)
    low = row8 < 4
    comp = lax.rem(row8, 4)
    is_xyz = comp < 3
    zero8 = jnp.zeros((8, ATOMS), F32)

    kinds = types_ref[...].reshape(8, ATOMS)
    table = jnp.zeros((8, ATOMS), F32)
    for kind in range(KINDS):
        table = jnp.where(kinds == kind, strength_ref[kind], table)
    lanes = lax.broadcasted_iota(jnp.int32, (1, ATOMS), 1)
    for cell in range(8):
        z, x, y = cell // 4, cell // 2 % 2, cell % 2
        live = (lanes < counts_ref[z, x, y]).astype(F32)
        live_ref[pl.ds(cell, 1), :] = live
        for k in range(3):
            region[0, 1 + z, 1 + x, y, pl.ds(k, 1), :] = pos_ref[k, z, x, pl.ds(y, 1), :]
            speed[cell // 2, pl.ds(4 * y + k, 1), :] = vel_ref[k, z, x, pl.ds(y, 1), :]
        region[0, 1 + z, 1 + x, y, pl.ds(3, 1), :] = table[cell : cell + 1] * live
        speed[cell // 2, pl.ds(4 * y + 3, 1), :] = jnp.zeros((1, ATOMS), F32)

    def halo_copies(slot):
        copies = []
        for i, d in enumerate(DIRECTIONS):
            (sz, tz), (sx, tx), (sy, ty) = spans(d[0]), spans(d[1]), spans_y(d[2])
            copies.append(
                pltpu.make_async_remote_copy(
                    src_ref=region.at[slot, sz, sx, sy],
                    dst_ref=region.at[slot, tz, tx, ty],
                    send_sem=send_sem.at[slot, i],
                    recv_sem=recv_sem.at[slot, i],
                    device_id=device(d),
                    device_id_type=MESH,
                )
            )
        return copies

    def static_parts():
        for z, x in itertools.product(range(4), range(4)):
            tiles = []
            for y in (0, 1, -1, 2):
                tile = zero8
                for cell in range(8):
                    o = (z - 1 - cell // 4, x - 1 - cell // 2 % 2, y - cell % 2)
                    if max(map(abs, o)) <= 1:
                        k = (o[0] + 1) * 9 + (o[1] + 1) * 3 + o[2] + 1
                        flag = pair_ref[k, cell // 4, cell // 2 % 2, cell % 2]
                        tile = jnp.where(row8 == cell, (flag.astype(F32) - 1.0) * 100.0, tile)
                tiles.append(tile)
            flag_ref[4 * z + x] = jnp.concatenate(tiles, axis=0).astype(BF16)
        for p in range(4):
            for t in range(3):
                for side in range(2):
                    half = ((0, 0), (1, 1), (0, 1))[t][side]
                    mark = jnp.where((low if half == 0 else ~low) & is_xyz, -1.0, 0.0)
                    pair = [mark, zero8] if t < 2 else [zero8, mark]
                    seat = ((0, 0), (1, 1), (2, 3))[t][side]
                    picks = [
                        jnp.where(row8 == 2 * p + side, 1.0, 0.0) if s == seat else zero8
                        for s in range(4)
                    ]
                    right_ref[p, t, 96:144, pl.ds(128 * side, 128)] = jnp.concatenate(
                        pair * 3, axis=0
                    ).astype(BF16)
                    right_ref[p, t, 160:192, pl.ds(128 * side, 128)] = jnp.concatenate(
                        picks, axis=0
                    ).astype(BF16)

    def shift_of(z, x, part):
        y_low, y_high = ((-1.0, 0.0), (-2.0, 1.0))[part]
        y = jnp.where(low, y_low, y_high)
        return jnp.where(
            comp == 0, z - 2.0, jnp.where(comp == 1, x - 2.0, jnp.where(comp == 2, y, 0.0))
        )

    def own_tile(slot, z, x, part):
        return jnp.concatenate(
            [region[slot, z, x, 2 * part], region[slot, z, x, 2 * part + 1]], axis=0
        )

    def strength_rows(tile):
        return jnp.concatenate(
            [
                jnp.broadcast_to(tile[3:4], (4, ATOMS)),
                jnp.broadcast_to(tile[7:8], (4, ATOMS)),
            ],
            axis=0,
        )

    def build_left(slot, z, x, both):
        column = 4 * z + x
        parts = []
        for part in range(2):
            if part == 1 and not both:
                parts.append([zero8] * 6)
                continue
            raw = own_tile(slot, z, x, part)
            tile = raw + shift_of(z, x, part)
            parts.append(list(thirds(tile)) + list(thirds(tile * tile)))
            value = jnp.where(is_xyz, tile, 1.0) * strength_rows(raw)
            high = value.astype(BF16).astype(F32)
            value_ref[part, :, pl.ds(128 * column, 128)] = jnp.concatenate(
                [high, value - high], axis=0
            ).astype(BF16)
        rows = []
        for kind in (0, 0, 1, 1, 0, 2, 3, 4, 5):
            rows += [parts[0][kind], parts[1][kind]]
        rows += [jnp.ones((16, ATOMS), F32)]
        stack = jnp.concatenate(
            [jnp.concatenate(rows, axis=0).astype(BF16), flag_ref[column]], axis=0
        )
        left_ref[column] = stack.T

    def build_right(slot):
        for p in range(4):
            z, x = 1 + p // 2, 1 + p % 2
            tile = own_tile(slot, z, x, 0) + shift_of(z, x, 0)
            tile = jnp.where(is_xyz, tile, 0.0)
            high, mid, rest = (2.0 * v for v in thirds(tile))
            terms = [high, mid, high, mid, rest, high]
            swapped = [swap_halves(v) for v in (high, mid, rest)]
            swapped = [swapped[i] for i in (0, 1, 0, 1, 2, 0)]
            squares = [-v for v in thirds(tile * tile)]
            squares_swapped = [swap_halves(v) for v in squares]
            for side in range(2):
                a, b = (squares, squares_swapped) if side == 0 else (squares_swapped, squares)
                ones_rows = jnp.concatenate(
                    [
                        jnp.where(low, jnp.where(is_xyz, a[0], 1.0), b[1]),
                        jnp.where(low, a[2], 0.0),
                    ],
                    axis=0,
                ).astype(BF16)
                for t in range(3):
                    half = ((0, 0), (1, 1), (0, 1))[t][side]
                    source = terms if half == side else swapped
                    keep = low if half == 0 else ~low
                    rows = []
                    for v in source:
                        v = jnp.where(keep, v, 0.0)
                        rows += [v, zero8] if t < 2 else [zero8, v]
                    at = pl.ds(128 * side, 128)
                    right_ref[p, t, 0:96, at] = jnp.concatenate(rows, axis=0).astype(BF16)
                    right_ref[p, t, 144:160, at] = ones_rows

    def add_pairs(p, t, columns, first):
        lhs = jnp.concatenate([left_ref[c] for c in columns], axis=0)
        near = jnp.dot(lhs, right_ref[p, t], preferred_element_type=F32)
        near = jnp.maximum(near, 0.0)
        weight = near * near
        high = weight.astype(BF16)
        rest = (weight - high.astype(F32)).astype(BF16)
        part = 0 if t < 2 else 1
        values = jnp.concatenate(
            [value_ref[part, :, pl.ds(128 * c, 128)] for c in columns], axis=1
        )
        add = jnp.dot(values, high, preferred_element_type=F32) + jnp.dot(
            values, rest, preferred_element_type=F32
        )
        if first:
            total[p, t] = add
        else:
            total[p, t] += add

    def update(slot):
        for p in range(4):
            z, x = 1 + p // 2, 1 + p % 2
            both = total[p, 0]
            both = both[:8] + both[8:]
            other = total[p, 1]
            other = other[:8] + other[8:]
            apart = total[p, 2]
            apart = apart[:8] + apart[8:]
            sums = jnp.concatenate(
                [
                    both[:4, :128] + other[4:, :128] + apart[:4, :128],
                    both[:4, 128:] + other[4:, 128:] + apart[4:, 128:],
                ],
                axis=0,
            )
            raw = own_tile(slot, z, x, 0)
            tile = raw + shift_of(z, x, 0)
            force = -6.0 * strength_rows(raw) * (sums - tile * strength_rows(sums))
            new_speed = speed[p] + STEP_TIME * jnp.where(is_xyz, force, 0.0)
            speed[p] = new_speed
            new = raw + STEP_TIME * new_speed
            region[slot + 1, z, x, 0] = new[:4]
            region[slot + 1, z, x, 1] = new[4:]

    own = [(z, x) for z in (1, 2) for x in (1, 2)]

    def one_step(slot, carry):
        copies = halo_copies(slot)
        for copy in copies:
            copy.start()
        build_right(slot)
        for z, x in own:
            build_left(slot, z, x, False)
        for p in range(4):
            for t in range(2):
                add_pairs(p, t, [5, 6, 9, 10], True)
        for copy in copies[:NEAR]:
            copy.wait_recv()
        for z in (1, 2):
            for x in range(4):
                build_left(slot, z, x, True)
        for p in range(4):
            az, ax = p // 2, p % 2
            x = 3 * ax
            for t in range(2):
                add_pairs(p, t, [4 + x, 8 + x], False)
            add_pairs(p, 2, [4 * z + ax + i for z in (1, 2) for i in range(3)], True)
        for copy in copies[NEAR:]:
            copy.wait_recv()
        for z in (0, 3):
            for x in range(4):
                build_left(slot, z, x, True)
        for p in range(4):
            az, ax = p // 2, p % 2
            for t in range(3):
                add_pairs(p, t, [12 * az + ax + i for i in range(3)], False)
        update(slot)
        for copy in copies:
            copy.wait_send()
        return carry

    static_parts()
    pl.semaphore_wait(barrier, len(greeted))
    lax.fori_loop(0, STEPS, one_step, 0)

    myself = (me_z * n_x + me_x) * n_y + me_y
    states, seats = [], []
    for cell in range(8):
        z, x, y = cell // 4, cell // 2 % 2, cell % 2
        moved = jnp.concatenate(
            [region[STEPS, 1 + z, 1 + x, y], speed[cell // 2, 4 * y : 4 * y + 4]], axis=0
        )
        live = jnp.broadcast_to(live_ref[pl.ds(cell, 1), :], (8, ATOMS))
        states.append(jnp.where(is_xyz, moved * live, 0.0))
        seats.append(dest_ref[z, x, y])
    moves = []
    for r, d in enumerate(peers):
        target = device(d)
        base = ((target[0] * n_x + target[1]) * n_y + target[2]) * SEATS
        message = jnp.where(row8 == 3, -1.0, 0.0)
        for cell in range(8):
            seat = seats[cell] - base
            hit = jnp.logical_and(seat >= 0, seat < SEATS)
            tagged = jnp.where(row8 == 3, seat.astype(F32), states[cell])
            message = jnp.where(hit, tagged, message)
        send_box[r] = message
        move = pltpu.make_async_remote_copy(
            src_ref=send_box.at[r],
            dst_ref=box.at[r],
            send_sem=move_send_sem.at[r],
            recv_sem=move_recv_sem.at[r],
            device_id=target,
            device_id_type=MESH,
        )
        move.start()
        moves.append(move)
    results = []
    for seat in range(SEATS):
        result = zero8
        for cell in range(8):
            result = jnp.where(seats[cell] == myself * SEATS + seat, states[cell], result)
        results.append(result)
    for move in moves:
        move.wait_recv()
    messages = [box[r] for r in range(7)]
    marks = [jnp.broadcast_to(m[3:4], (8, ATOMS)) for m in messages]
    for seat in range(SEATS):
        result = results[seat]
        for r in range(7):
            result = jnp.where(marks[r] == float(seat), messages[r], result)
        for k in range(3):
            out_pos_ref[k, pl.ds(seat, 1), :] = result[k : k + 1]
            out_vel_ref[k, pl.ds(seat, 1), :] = result[4 + k : 5 + k]
    for move in moves:
        move.wait_send()


def on_device(positions, velocities, types, strength, counts, pair_list, destination):
    vmem = pl.BlockSpec(memory_space=pltpu.VMEM)
    smem = pl.BlockSpec(memory_space=pltpu.SMEM)
    shape = jax.ShapeDtypeStruct((3, SEATS, ATOMS), F32)
    return pl.pallas_call(
        body,
        out_shape=(shape, shape),
        in_specs=[vmem, vmem, vmem, smem, smem, smem, smem],
        out_specs=(vmem, vmem),
        scratch_shapes=[
            pltpu.VMEM((STEPS + 1, 4, 4, 4, 4, ATOMS), F32),
            pltpu.VMEM((4, 8, ATOMS), F32),
            pltpu.VMEM((8, ATOMS), F32),
            pltpu.VMEM((16, 32, ATOMS), BF16),
            pltpu.VMEM((16, ATOMS, DEPTH), BF16),
            pltpu.VMEM((4, 3, DEPTH, 2 * ATOMS), BF16),
            pltpu.VMEM((2, 16, 16 * ATOMS), BF16),
            pltpu.VMEM((4, 3, 16, 2 * ATOMS), F32),
            pltpu.VMEM((7, 8, ATOMS), F32),
            pltpu.VMEM((7, 8, ATOMS), F32),
            pltpu.SemaphoreType.DMA((STEPS, 26)),
            pltpu.SemaphoreType.DMA((STEPS, 26)),
            pltpu.SemaphoreType.DMA((7,)),
            pltpu.SemaphoreType.DMA((7,)),
        ],
        compiler_params=pltpu.CompilerParams(collective_id=0, has_side_effects=True),
    )(positions, velocities, types, strength, counts, pair_list, destination)


def solution(mesh):
    return jax.shard_map(
        on_device,
        mesh=mesh,
        in_specs=(
            P(None, "tower", "px", "py", None),
            P(None, "tower", "px", "py", None),
            P("tower", "px", "py", None),
            P(),
            P("tower", "px", "py"),
            P(None, "tower", "px", "py"),
            P("tower", "px", "py"),
        ),
        out_specs=(P(None, ("tower", "px", "py"), None), P(None, ("tower", "px", "py"), None)),
        check_vma=False,
    )
```

```python
import itertools

import jax
import jax.numpy as jnp
from jax import lax
from jax.experimental import pallas as pl
from jax.experimental.pallas import tpu as pltpu
from jax.sharding import PartitionSpec as P

STEPS = 4
STEP_TIME = 0.02
KINDS = 16
SEATS = 15
ATOMS = 128
DEPTH = 176
MESH = pl.DeviceIdType.MESH
F32 = jnp.float32
BF16 = jnp.bfloat16

DIRECTIONS = sorted(
    (d for d in itertools.product((-1, 0, 1), repeat=3) if d != (0, 0, 0)),
    key=lambda d: abs(d[0]),
)
NEAR = 8
SEAT_OF_Y = {0: 0, 1: 1, -1: 2, 2: 3}


def spans(step):
    if step == 0:
        return pl.ds(1, 2), pl.ds(1, 2)
    return (pl.ds(2, 1), pl.ds(0, 1)) if step == 1 else (pl.ds(1, 1), pl.ds(3, 1))


def spans_y(step):
    if step == 0:
        return pl.ds(0, 2), pl.ds(0, 2)
    return (pl.ds(1, 1), pl.ds(2, 1)) if step == 1 else (pl.ds(0, 1), pl.ds(3, 1))


def thirds(x):
    high = x.astype(BF16).astype(F32)
    rest = x - high
    mid = rest.astype(BF16).astype(F32)
    return high, mid, rest - mid


def swap_halves(x):
    return jnp.concatenate([x[4:], x[:4]], axis=0)


def host_of(t, x, y):
    return (2 * (t // 2) + y // 4, x, 2 * lax.rem(y, 4) + lax.rem(t, 2))


def body(
    pos_ref, vel_ref, types_ref, strength_ref, counts_ref, pair_ref, dest_ref,
    out_pos_ref, out_vel_ref,
    region, speed, seat_ref, parcel, hosted, flag_ref, left_ref, right_ref, value_ref, total,
    box, stay_box, send_box, stay_send,
    send_sem, recv_sem, host_sem, move_send_sem, move_recv_sem,
):
    home_t, home_x, home_y = (lax.axis_index(a) for a in ("tower", "px", "py"))
    n_z, n_x, n_y = (lax.axis_size(a) for a in ("tower", "px", "py"))
    me_z = 2 * (home_t // 2) + lax.rem(home_y, 2)
    me_x = home_x
    me_y = 4 * lax.rem(home_t, 2) + home_y // 2
    host = host_of(home_t, home_x, home_y)
    same_tower = me_z == home_t
    at_home = jnp.logical_and(same_tower, me_y == home_y)

    def device(d):
        return host_of(
            lax.rem(me_z + d[0] + n_z, n_z),
            lax.rem(me_x + d[1] + n_x, n_x),
            lax.rem(me_y + d[2] + n_y, n_y),
        )

    def shift_y(y, r):
        return lax.rem(y + r + n_y, n_y)

    def goes_to_itself(r):
        return jnp.logical_and(same_tower, shift_y(me_y, r) == home_y)

    barrier = pltpu.get_barrier_semaphore()

    def greet(target):
        pl.semaphore_signal(barrier, inc=1, device_id=target, device_id_type=MESH)

    @pl.when(jnp.logical_not(at_home))
    def _():
        greet((me_z, me_x, me_y))

    for d in DIRECTIONS:
        greet(device(d))
    for r in range(8):

        @pl.when(jnp.logical_not(goes_to_itself(r)))
        def _():
            greet(host_of(home_t, home_x, shift_y(home_y, -r)))

    expected = len(DIRECTIONS) + 9 - at_home.astype(jnp.int32) - same_tower.astype(jnp.int32)

    row8 = lax.broadcasted_iota(jnp.int32, (8, ATOMS), 0)
    row16 = lax.broadcasted_iota(jnp.int32, (16, ATOMS), 0)
    low = row8 < 4
    comp = lax.rem(row8, 4)
    is_xyz = comp < 3
    zero8 = jnp.zeros((8, ATOMS), F32)

    kinds = types_ref[...].reshape(8, ATOMS)
    table = jnp.zeros((8, ATOMS), F32)
    for kind in range(KINDS):
        table = jnp.where(kinds == kind, strength_ref[kind], table)
    lanes = lax.broadcasted_iota(jnp.int32, (1, ATOMS), 1)
    parcel[8] = zero8
    for cell in range(8):
        z, x, y = cell // 4, cell // 2 % 2, cell % 2
        live = (lanes < counts_ref[z, x, y]).astype(F32)
        for k in range(3):
            parcel[cell, pl.ds(k, 1), :] = pos_ref[k, z, x, pl.ds(y, 1), :]
            parcel[cell, pl.ds(4 + k, 1), :] = vel_ref[k, z, x, pl.ds(y, 1), :]
        parcel[cell, pl.ds(3, 1), :] = table[cell : cell + 1] * live
        seat = dest_ref[z, x, y].astype(F32)
        parcel[cell, pl.ds(7, 1), :] = jnp.full((1, ATOMS), seat, F32)
        parcel[8, pl.ds(cell, 1), pl.ds(0, 27)] = pair_ref[z, x, pl.ds(y, 1), :].astype(F32)
    delivery = pltpu.make_async_remote_copy(
        src_ref=parcel,
        dst_ref=hosted,
        send_sem=host_sem.at[0],
        recv_sem=host_sem.at[1],
        device_id=host,
        device_id_type=MESH,
    )

    def halo_copies(slot):
        copies = []
        for i, d in enumerate(DIRECTIONS):
            (sz, tz), (sx, tx), (sy, ty) = spans(d[0]), spans(d[1]), spans_y(d[2])
            copies.append(
                pltpu.make_async_remote_copy(
                    src_ref=region.at[slot, sz, sx, sy],
                    dst_ref=region.at[slot, tz, tx, ty],
                    send_sem=send_sem.at[slot, i],
                    recv_sem=recv_sem.at[slot, i],
                    device_id=device(d),
                    device_id_type=MESH,
                )
            )
        return copies

    def constant_parts():
        for p in range(4):
            for t in range(3):
                for side in range(2):
                    half = ((0, 0), (1, 1), (0, 1))[t][side]
                    mark = jnp.where((low if half == 0 else ~low) & is_xyz, -1.0, 0.0)
                    pair = [mark, zero8] if t < 2 else [zero8, mark]
                    right_ref[p, t, 96:144, pl.ds(128 * side, 128)] = jnp.concatenate(
                        pair * 3, axis=0
                    ).astype(BF16)

    def unpack():
        for cell in range(8):
            z, x, y = cell // 4, cell // 2 % 2, cell % 2
            tile = hosted[cell]
            region[0, 1 + z, 1 + x, y] = tile[:4]
            speed[cell // 2, pl.ds(4 * y, 4), :] = jnp.where(row8[:4] < 3, tile[4:], 0.0)
            seat_ref[cell] = jnp.broadcast_to(tile[7:8], (8, ATOMS))
        padded = jnp.concatenate([(hosted[8] - 1.0) * 100.0] + [zero8] * 15, axis=0)
        turned = padded.T
        for cell in range(8):
            flag_ref[cell] = jnp.broadcast_to(turned[:32, cell : cell + 1], (32, ATOMS))
        for p, side in itertools.product(range(4), range(2)):
            cell, z, x = 2 * p + side, p // 2, p % 2
            rows32 = flag_ref[cell]
            for t in range(3):
                y = ((0, 0), (1, 1), (-1, 2))[t][side] - side + 1
                rows = [jnp.zeros((1, ATOMS), F32)] * 16
                for oz, ox in itertools.product(range(3), range(3)):
                    k = 9 * oz + 3 * ox + y
                    rows[4 * (z + oz) + x + ox] = rows32[k : k + 1]
                right_ref[p, t, 160:176, pl.ds(128 * side, 128)] = jnp.concatenate(
                    rows, axis=0
                ).astype(BF16)

    def shift_of(z, x, part):
        y_low, y_high = ((-1.0, 0.0), (-2.0, 1.0))[part]
        y = jnp.where(low, y_low, y_high)
        return jnp.where(
            comp == 0, z - 2.0, jnp.where(comp == 1, x - 2.0, jnp.where(comp == 2, y, 0.0))
        )

    def own_tile(slot, z, x, part):
        return jnp.concatenate(
            [region[slot, z, x, 2 * part], region[slot, z, x, 2 * part + 1]], axis=0
        )

    def strength_rows(tile):
        return jnp.concatenate(
            [
                jnp.broadcast_to(tile[3:4], (4, ATOMS)),
                jnp.broadcast_to(tile[7:8], (4, ATOMS)),
            ],
            axis=0,
        )

    def build_left(slot, z, x, both):
        column = 4 * z + x
        parts = []
        for part in range(2):
            if part == 1 and not both:
                parts.append([zero8] * 6)
                continue
            raw = own_tile(slot, z, x, part)
            tile = raw + shift_of(z, x, part)
            parts.append(list(thirds(tile)) + list(thirds(tile * tile)))
            value = jnp.where(is_xyz, tile, 1.0) * strength_rows(raw)
            high = value.astype(BF16).astype(F32)
            value_ref[part, :, pl.ds(128 * column, 128)] = jnp.concatenate(
                [high, value - high], axis=0
            ).astype(BF16)
        rows = []
        for kind in (0, 0, 1, 1, 0, 2, 3, 4, 5):
            rows += [parts[0][kind], parts[1][kind]]
        rows += [jnp.ones((16, ATOMS), F32), jnp.where(row16 == column, 1.0, 0.0)]
        left_ref[column] = jnp.concatenate(rows, axis=0).astype(BF16).T

    def build_right(slot):
        for p in range(4):
            z, x = 1 + p // 2, 1 + p % 2
            tile = own_tile(slot, z, x, 0) + shift_of(z, x, 0)
            tile = jnp.where(is_xyz, tile, 0.0)
            high, mid, rest = (2.0 * v for v in thirds(tile))
            terms = [high, mid, high, mid, rest, high]
            swapped = [swap_halves(v) for v in (high, mid, rest)]
            swapped = [swapped[i] for i in (0, 1, 0, 1, 2, 0)]
            squares = [-v for v in thirds(tile * tile)]
            squares_swapped = [swap_halves(v) for v in squares]
            for side in range(2):
                a, b = (squares, squares_swapped) if side == 0 else (squares_swapped, squares)
                ones_rows = jnp.concatenate(
                    [
                        jnp.where(low, jnp.where(is_xyz, a[0], 1.0), b[1]),
                        jnp.where(low, a[2], 0.0),
                    ],
                    axis=0,
                ).astype(BF16)
                for t in range(3):
                    half = ((0, 0), (1, 1), (0, 1))[t][side]
                    source = terms if half == side else swapped
                    keep = low if half == 0 else ~low
                    rows = []
                    for v in source:
                        v = jnp.where(keep, v, 0.0)
                        rows += [v, zero8] if t < 2 else [zero8, v]
                    at = pl.ds(128 * side, 128)
                    right_ref[p, t, 0:96, at] = jnp.concatenate(rows, axis=0).astype(BF16)
                    right_ref[p, t, 144:160, at] = ones_rows

    def add_pairs(p, t, columns, first):
        lhs = jnp.concatenate([left_ref[c] for c in columns], axis=0)
        near = jnp.dot(lhs, right_ref[p, t], preferred_element_type=F32)
        near = jnp.maximum(near, 0.0)
        weight = near * near
        high = weight.astype(BF16)
        rest = (weight - high.astype(F32)).astype(BF16)
        part = 0 if t < 2 else 1
        values = jnp.concatenate(
            [value_ref[part, :, pl.ds(128 * c, 128)] for c in columns], axis=1
        )
        add = jnp.dot(values, high, preferred_element_type=F32) + jnp.dot(
            values, rest, preferred_element_type=F32
        )
        if first:
            total[p, t] = add
        else:
            total[p, t] += add

    def update(slot):
        for p in range(4):
            z, x = 1 + p // 2, 1 + p % 2
            both = total[p, 0]
            both = both[:8] + both[8:]
            other = total[p, 1]
            other = other[:8] + other[8:]
            apart = total[p, 2]
            apart = apart[:8] + apart[8:]
            sums = jnp.concatenate(
                [
                    both[:4, :128] + other[4:, :128] + apart[:4, :128],
                    both[:4, 128:] + other[4:, 128:] + apart[4:, 128:],
                ],
                axis=0,
            )
            raw = own_tile(slot, z, x, 0)
            tile = raw + shift_of(z, x, 0)
            force = -6.0 * strength_rows(raw) * (sums - tile * strength_rows(sums))
            new_speed = speed[p] + STEP_TIME * jnp.where(is_xyz, force, 0.0)
            speed[p] = new_speed
            new = raw + STEP_TIME * new_speed
            region[slot + 1, z, x, 0] = new[:4]
            region[slot + 1, z, x, 1] = new[4:]

    own = [(z, x) for z in (1, 2) for x in (1, 2)]

    def one_step(slot, carry):
        copies = halo_copies(slot)
        for copy in copies:
            copy.start()
        build_right(slot)
        for z, x in own:
            build_left(slot, z, x, False)
        for p in range(4):
            for t in range(2):
                add_pairs(p, t, [5, 6, 9, 10], True)
        for copy in copies[:NEAR]:
            copy.wait_recv()
        for z in (1, 2):
            for x in range(4):
                build_left(slot, z, x, True)
        for p in range(4):
            az, ax = p // 2, p % 2
            x = 3 * ax
            for t in range(2):
                add_pairs(p, t, [4 + x, 8 + x], False)
            add_pairs(p, 2, [4 * z + ax + i for z in (1, 2) for i in range(3)], True)
        for copy in copies[NEAR:]:
            copy.wait_recv()
        for z in (0, 3):
            for x in range(4):
                build_left(slot, z, x, True)
        for p in range(4):
            az, ax = p // 2, p % 2
            for t in range(3):
                add_pairs(p, t, [12 * az + ax + i for i in range(3)], False)
        update(slot)
        for copy in copies:
            copy.wait_send()
        return carry

    constant_parts()
    pl.semaphore_wait(barrier, expected)

    @pl.when(jnp.logical_not(at_home))
    def _():
        delivery.start()
        delivery.wait_recv()
        delivery.wait_send()

    @pl.when(at_home)
    def _():
        hosted[...] = parcel[...]

    unpack()
    lax.fori_loop(0, STEPS, one_step, 0)

    states, moves = [], []
    for cell in range(8):
        z, x, y = cell // 4, cell // 2 % 2, cell % 2
        here = region[STEPS, 1 + z, 1 + x, y]
        moved = jnp.concatenate([here, speed[cell // 2, 4 * y : 4 * y + 4]], axis=0)
        live = jnp.broadcast_to(here[3:4], (8, ATOMS)) > 0.0
        states.append(jnp.where(live & is_xyz, moved, 0.0))
    for r in range(8):
        y = shift_y(me_y, r)
        base = (((me_z * n_x + me_x) * n_y + y) * SEATS).astype(F32)
        message = jnp.where(row8 == 3, -1.0, 0.0)
        for cell in range(8):
            seat = seat_ref[cell] - base
            hit = (seat >= 0.0) & (seat < float(SEATS))
            tagged = jnp.where(row8 == 3, seat, states[cell])
            if r == 0:
                stay_send[cell] = jnp.where(hit, tagged, jnp.where(row8 == 3, -1.0, 0.0))
            else:
                message = jnp.where(hit, tagged, message)
        if r > 0:
            send_box[r - 1] = message
        src, dst = (stay_send, stay_box) if r == 0 else (send_box.at[r - 1], box.at[r - 1])
        move = pltpu.make_async_remote_copy(
            src_ref=src,
            dst_ref=dst,
            send_sem=move_send_sem.at[r],
            recv_sem=move_recv_sem.at[r],
            device_id=(me_z, me_x, y),
            device_id_type=MESH,
        )
        moves.append(move)

        @pl.when(jnp.logical_not(goes_to_itself(r)))
        def _():
            move.start()

        @pl.when(goes_to_itself(r))
        def _():
            dst[...] = src[...]

    for r in range(8):

        @pl.when(jnp.logical_not(goes_to_itself(r)))
        def _():
            moves[r].wait_recv()

    messages = [stay_box[cell] for cell in range(8)] + [box[r] for r in range(7)]
    marks = [jnp.broadcast_to(m[3:4], (8, ATOMS)) for m in messages]
    for seat in range(SEATS):
        result = zero8
        for mark, message in zip(marks, messages):
            result = jnp.where(mark == float(seat), message, result)
        for k in range(3):
            out_pos_ref[k, pl.ds(seat, 1), :] = result[k : k + 1]
            out_vel_ref[k, pl.ds(seat, 1), :] = result[4 + k : 5 + k]
    for r in range(8):

        @pl.when(jnp.logical_not(goes_to_itself(r)))
        def _():
            moves[r].wait_send()


def on_device(positions, velocities, types, strength, counts, pair_list, destination):
    vmem = pl.BlockSpec(memory_space=pltpu.VMEM)
    smem = pl.BlockSpec(memory_space=pltpu.SMEM)
    shape = jax.ShapeDtypeStruct((3, SEATS, ATOMS), F32)
    return pl.pallas_call(
        body,
        out_shape=(shape, shape),
        in_specs=[vmem, vmem, vmem, smem, smem, vmem, smem],
        out_specs=(vmem, vmem),
        scratch_shapes=[
            pltpu.VMEM((STEPS + 1, 4, 4, 4, 4, ATOMS), F32),
            pltpu.VMEM((4, 8, ATOMS), F32),
            pltpu.VMEM((8, 8, ATOMS), F32),
            pltpu.VMEM((9, 8, ATOMS), F32),
            pltpu.VMEM((9, 8, ATOMS), F32),
            pltpu.VMEM((8, 32, ATOMS), F32),
            pltpu.VMEM((16, ATOMS, DEPTH), BF16),
            pltpu.VMEM((4, 3, DEPTH, 2 * ATOMS), BF16),
            pltpu.VMEM((2, 16, 16 * ATOMS), BF16),
            pltpu.VMEM((4, 3, 16, 2 * ATOMS), F32),
            pltpu.VMEM((7, 8, ATOMS), F32),
            pltpu.VMEM((8, 8, ATOMS), F32),
            pltpu.VMEM((7, 8, ATOMS), F32),
            pltpu.VMEM((8, 8, ATOMS), F32),
            pltpu.SemaphoreType.DMA((STEPS, 26)),
            pltpu.SemaphoreType.DMA((STEPS, 26)),
            pltpu.SemaphoreType.DMA((2,)),
            pltpu.SemaphoreType.DMA((8,)),
            pltpu.SemaphoreType.DMA((8,)),
        ],
        compiler_params=pltpu.CompilerParams(collective_id=0, has_side_effects=True),
    )(positions, velocities, types, strength, counts, pair_list.transpose(1, 2, 3, 0), destination)


def solution(mesh):
    return jax.shard_map(
        on_device,
        mesh=mesh,
        in_specs=(
            P(None, "tower", "px", "py", None),
            P(None, "tower", "px", "py", None),
            P("tower", "px", "py", None),
            P(),
            P("tower", "px", "py"),
            P(None, "tower", "px", "py"),
            P("tower", "px", "py"),
        ),
        out_specs=(P(None, ("tower", "px", "py"), None), P(None, ("tower", "px", "py"), None)),
        check_vma=False,
    )
```

```python
import itertools

import jax
import jax.numpy as jnp
from jax import lax
from jax.experimental import pallas as pl
from jax.experimental.pallas import tpu as pltpu
from jax.sharding import PartitionSpec as P

STEPS = 4
STEP_TIME = 0.02
KINDS = 16
SEATS = 15
ATOMS = 128
DEPTH = 112
CHUNK, AHEAD = 2, 2
MESH = pl.DeviceIdType.MESH
F32 = jnp.float32
BF16 = jnp.bfloat16

DIRECTIONS = sorted(
    (d for d in itertools.product((-1, 0, 1), repeat=3) if d != (0, 0, 0)),
    key=lambda d: (sum(map(abs, d)), abs(d[1]) + abs(d[2])),
)
NEAREST, FACES, EDGES = 2, 6, 18
SEAT_OF_Y = {0: 0, 1: 1, -1: 2, 2: 3}


def spans(step):
    if step == 0:
        return pl.ds(1, 2), pl.ds(1, 2)
    return (pl.ds(2, 1), pl.ds(0, 1)) if step == 1 else (pl.ds(1, 1), pl.ds(3, 1))


def spans_y(step):
    if step == 0:
        return pl.ds(0, 2), pl.ds(0, 2)
    return (pl.ds(1, 1), pl.ds(2, 1)) if step == 1 else (pl.ds(0, 1), pl.ds(3, 1))


def thirds(x):
    high = x.astype(BF16).astype(F32)
    rest = x - high
    mid = rest.astype(BF16).astype(F32)
    return high, mid, rest - mid


def swap_halves(x):
    return jnp.concatenate([x[4:], x[:4]], axis=0)


def host_of(t, x, y):
    return (2 * (t // 2) + y // 4, x, 2 * lax.rem(y, 4) + lax.rem(t, 2))


def body(
    pos_ref, vel_ref, types_ref, strength_ref, counts_ref, pair_ref, dest_ref,
    out_pos_ref, out_vel_ref,
    region, speed, seat_ref, parcel, hosted, flag_ref, left_ref, right_ref, value_ref, total,
    box, stay_box, send_box, stay_send,
    send_sem, recv_sem, host_sem, move_send_sem, move_recv_sem,
):
    home_t, home_x, home_y = (lax.axis_index(a) for a in ("tower", "px", "py"))
    n_z, n_x, n_y = (lax.axis_size(a) for a in ("tower", "px", "py"))
    me_z = 2 * (home_t // 2) + lax.rem(home_y, 2)
    me_x = home_x
    me_y = 4 * lax.rem(home_t, 2) + home_y // 2
    host = host_of(home_t, home_x, home_y)
    same_tower = me_z == home_t
    at_home = jnp.logical_and(same_tower, me_y == home_y)

    def device(d):
        return host_of(
            lax.rem(me_z + d[0] + n_z, n_z),
            lax.rem(me_x + d[1] + n_x, n_x),
            lax.rem(me_y + d[2] + n_y, n_y),
        )

    def shift_y(y, r):
        return lax.rem(y + r + n_y, n_y)

    def goes_to_itself(r):
        return jnp.logical_and(same_tower, shift_y(me_y, r) == home_y)

    barrier = pltpu.get_barrier_semaphore()

    def greet(target):
        pl.semaphore_signal(barrier, inc=1, device_id=target, device_id_type=MESH)

    @pl.when(jnp.logical_not(at_home))
    def _():
        greet((me_z, me_x, me_y))

    for d in DIRECTIONS:
        greet(device(d))
    for r in range(8):

        @pl.when(jnp.logical_not(goes_to_itself(r)))
        def _():
            greet(host_of(home_t, home_x, shift_y(home_y, -r)))

    expected = len(DIRECTIONS) + 9 - at_home.astype(jnp.int32) - same_tower.astype(jnp.int32)

    row8 = lax.broadcasted_iota(jnp.int32, (8, ATOMS), 0)
    row16 = lax.broadcasted_iota(jnp.int32, (16, ATOMS), 0)
    low = row8 < 4
    comp = lax.rem(row8, 4)
    is_xyz = comp < 3
    zero8 = jnp.zeros((8, ATOMS), F32)

    kinds = types_ref[...].reshape(8, ATOMS)
    table = jnp.zeros((8, ATOMS), F32)
    for kind in range(KINDS):
        table = jnp.where(kinds == kind, strength_ref[kind], table)
    lanes = lax.broadcasted_iota(jnp.int32, (1, ATOMS), 1)
    parcel[8] = zero8
    for cell in range(8):
        z, x, y = cell // 4, cell // 2 % 2, cell % 2
        live = (lanes < counts_ref[z, x, y]).astype(F32)
        for k in range(3):
            parcel[cell, pl.ds(k, 1), :] = pos_ref[k, z, x, pl.ds(y, 1), :]
            parcel[cell, pl.ds(4 + k, 1), :] = vel_ref[k, z, x, pl.ds(y, 1), :]
        parcel[cell, pl.ds(3, 1), :] = table[cell : cell + 1] * live
        seat = dest_ref[z, x, y].astype(F32)
        parcel[cell, pl.ds(7, 1), :] = jnp.full((1, ATOMS), seat, F32)
        parcel[8, pl.ds(cell, 1), pl.ds(0, 27)] = pair_ref[z, x, pl.ds(y, 1), :].astype(F32)
    delivery = pltpu.make_async_remote_copy(
        src_ref=parcel,
        dst_ref=hosted,
        send_sem=host_sem.at[0],
        recv_sem=host_sem.at[1],
        device_id=host,
        device_id_type=MESH,
    )

    def halo_copies(slot):
        copies = []
        for i, d in enumerate(DIRECTIONS):
            (sz, tz), (sx, tx), (sy, ty) = spans(d[0]), spans(d[1]), spans_y(d[2])
            copies.append(
                pltpu.make_async_remote_copy(
                    src_ref=region.at[slot, sz, sx, sy],
                    dst_ref=region.at[slot, tz, tx, ty],
                    send_sem=send_sem.at[slot, i],
                    recv_sem=recv_sem.at[slot, i],
                    device_id=device(d),
                    device_id_type=MESH,
                )
            )
        return copies

    def constant_parts():
        for p in range(4):
            for t in range(3):
                for side in range(2):
                    half = ((0, 0), (1, 1), (0, 1))[t][side]
                    mark = jnp.where((low if half == 0 else ~low) & is_xyz, -1.0, 0.0)
                    right_ref[p, 80:96, pl.ds(256 * t + 128 * side, 128)] = jnp.concatenate(
                        [mark, mark], axis=0
                    ).astype(BF16)

    def unpack():
        for cell in range(8):
            z, x, y = cell // 4, cell // 2 % 2, cell % 2
            tile = hosted[cell]
            region[0, 1 + z, 1 + x, y] = tile[:4]
            speed[cell // 2, pl.ds(4 * y, 4), :] = jnp.where(row8[:4] < 3, tile[4:], 0.0)
            seat_ref[cell] = jnp.broadcast_to(tile[7:8], (8, ATOMS))
        padded = jnp.concatenate([(hosted[8] - 1.0) * 100.0] + [zero8] * 15, axis=0)
        turned = padded.T
        for cell in range(8):
            flag_ref[cell] = jnp.broadcast_to(turned[:32, cell : cell + 1], (32, ATOMS))
        for p, side in itertools.product(range(4), range(2)):
            cell, z, x = 2 * p + side, p // 2, p % 2
            rows32 = flag_ref[cell]
            for t in range(3):
                y = ((0, 0), (1, 1), (-1, 2))[t][side] - side + 1
                rows = [jnp.zeros((1, ATOMS), F32)] * 16
                for oz, ox in itertools.product(range(3), range(3)):
                    k = 9 * oz + 3 * ox + y
                    rows[4 * (z + oz) + x + ox] = rows32[k : k + 1]
                right_ref[p, 96:112, pl.ds(256 * t + 128 * side, 128)] = jnp.concatenate(
                    rows, axis=0
                ).astype(BF16)

    def shift_of(z, x, part):
        y_low, y_high = ((-1.0, 0.0), (-2.0, 1.0))[part]
        y = jnp.where(low, y_low, y_high)
        return jnp.where(
            comp == 0, z - 2.0, jnp.where(comp == 1, x - 2.0, jnp.where(comp == 2, y, 0.0))
        )

    def own_tile(slot, z, x, part):
        return jnp.concatenate(
            [region[slot, z, x, 2 * part], region[slot, z, x, 2 * part + 1]], axis=0
        )

    def strength_rows(tile):
        return jnp.concatenate(
            [
                jnp.broadcast_to(tile[3:4], (4, ATOMS)),
                jnp.broadcast_to(tile[7:8], (4, ATOMS)),
            ],
            axis=0,
        )

    def build_left(slot, z, x, part):
        column = 4 * z + x
        raw = own_tile(slot, z, x, part)
        tile = raw + shift_of(z, x, part)
        high, mid, rest = thirds(tile)
        ones = jnp.ones((24, ATOMS), F32)
        rows = [high, high, mid, mid, high, rest, ones, *thirds(tile * tile)]
        rows += [jnp.where(row16 == column, 1.0, 0.0)]
        left_ref[part, column] = jnp.concatenate(rows, axis=0).astype(BF16).T
        value = jnp.where(is_xyz, tile, 1.0) * strength_rows(raw)
        high = value.astype(BF16).astype(F32)
        value_ref[part, :, pl.ds(128 * column, 128)] = jnp.concatenate(
            [high, value - high], axis=0
        ).astype(BF16)

    def build_right(slot):
        for p in range(4):
            z, x = 1 + p // 2, 1 + p % 2
            tile = own_tile(slot, z, x, 0) + shift_of(z, x, 0)
            tile = jnp.where(is_xyz, tile, 0.0)
            terms = [2.0 * v for v in thirds(tile)]
            swapped = [swap_halves(v) for v in terms]
            squares = [-v for v in thirds(tile * tile)]
            squares[0] = jnp.where(is_xyz, squares[0], 1.0)
            for side in range(2):
                mine = low if side == 0 else ~low
                norms = [jnp.where(mine, v, 0.0) for v in squares]
                for t in range(3):
                    half = ((0, 0), (1, 1), (0, 1))[t][side]
                    keep = low if half == 0 else ~low
                    source = terms if half == side else swapped
                    high, mid, rest = [jnp.where(keep, v, 0.0) for v in source]
                    mark = jnp.where(keep & is_xyz, -1.0, 0.0)
                    rows = [high, mid, high, mid, rest, high, *norms, mark]
                    right_ref[p, 0:80, pl.ds(256 * t + 128 * side, 128)] = jnp.concatenate(
                        rows, axis=0
                    ).astype(BF16)

    def nearness(part, columns, targets):
        lhs = jnp.concatenate([left_ref[part, c] for c in columns], axis=0)
        rhs = jnp.concatenate(
            [right_ref[p, :, pl.ds(256 * t, 256)] for p, t in targets], axis=1
        )
        return jnp.dot(lhs, rhs, preferred_element_type=F32)

    def add_sums(near, part, columns, targets, first):
        near = jnp.maximum(near, 0.0)
        weight = near * near
        high = weight.astype(BF16)
        rest = (weight - high.astype(F32)).astype(BF16)
        values = jnp.concatenate(
            [value_ref[part, :, pl.ds(128 * c, 128)] for c in columns], axis=1
        )
        add = jnp.dot(values, high, preferred_element_type=F32) + jnp.dot(
            values, rest, preferred_element_type=F32
        )
        for i, (p, t) in enumerate(targets):
            more = add[:, 256 * i : 256 * i + 256]
            if first:
                total[p, t] = more
            else:
                total[p, t] += more

    def add_pairs(groups):
        parts = [
            (part, columns[at : at + CHUNK], targets, first and at == 0)
            for part, columns, targets, first in groups
            for at in range(0, len(columns), CHUNK)
        ]
        waiting = []
        for group in parts:
            waiting.append((nearness(*group[:3]), *group))
            if len(waiting) > AHEAD:
                add_sums(*waiting.pop(0))
        for group in waiting:
            add_sums(*group)

    def update(slot):
        for p in range(4):
            z, x = 1 + p // 2, 1 + p % 2
            both = total[p, 0]
            both = both[:8] + both[8:]
            other = total[p, 1]
            other = other[:8] + other[8:]
            apart = total[p, 2]
            apart = apart[:8] + apart[8:]
            sums = jnp.concatenate(
                [
                    both[:4, :128] + other[4:, :128] + apart[:4, :128],
                    both[:4, 128:] + other[4:, 128:] + apart[4:, 128:],
                ],
                axis=0,
            )
            raw = own_tile(slot, z, x, 0)
            tile = raw + shift_of(z, x, 0)
            force = -6.0 * strength_rows(raw) * (sums - tile * strength_rows(sums))
            new_speed = speed[p] + STEP_TIME * jnp.where(is_xyz, force, 0.0)
            speed[p] = new_speed
            new = raw + STEP_TIME * new_speed
            region[slot + 1, z, x, 0] = new[:4]
            region[slot + 1, z, x, 1] = new[4:]

    inner = (1, 2)
    own = [(z, x) for z in inner for x in inner]
    beside = [(z, x) for z in (0, 3) for x in inner] + [(z, x) for z in inner for x in (0, 3)]
    across = [(z, x) for z in (0, 3) for x in (0, 3)]

    def one_step(slot, carry):
        copies = halo_copies(slot)
        for copy in copies:
            copy.start()
        build_right(slot)
        for z, x in own:
            build_left(slot, z, x, 0)
        add_pairs([(0, [5, 6, 9, 10], [(p, 0), (p, 1)], True) for p in range(4)])
        for copy in copies[:NEAREST]:
            copy.wait_recv()
        for z in (0, 3):
            for x in inner:
                build_left(slot, z, x, 0)
        add_pairs(
            [
                (0, [12 * (p // 2) + 1, 12 * (p // 2) + 2], [(p, 0), (p, 1)], False)
                for p in range(4)
            ]
        )
        for copy in copies[NEAREST:FACES]:
            copy.wait_recv()
        for z, x in own:
            build_left(slot, z, x, 1)
        for z in inner:
            for x in (0, 3):
                build_left(slot, z, x, 0)
        add_pairs(
            [(1, [5, 6, 9, 10], [(p, 2), (p + 1, 2)], True) for p in (0, 2)]
            + [
                (0, [4 + 3 * (p % 2), 8 + 3 * (p % 2)], [(p, 0), (p, 1)], False)
                for p in range(4)
            ]
        )
        for copy in copies[FACES:EDGES]:
            copy.wait_recv()
        for z, x in beside:
            build_left(slot, z, x, 1)
        for z, x in across:
            build_left(slot, z, x, 0)
        add_pairs(
            [(1, [12 * i + 1, 12 * i + 2], [(2 * i, 2), (2 * i + 1, 2)], False) for i in (0, 1)]
            + [(1, [4 + 3 * i, 8 + 3 * i], [(i, 2), (2 + i, 2)], False) for i in (0, 1)]
            + [
                (0, [12 * (p // 2) + 3 * (p % 2)], [(p, 0), (p, 1)], False)
                for p in range(4)
            ]
        )
        for copy in copies[EDGES:]:
            copy.wait_recv()
        for z, x in across:
            build_left(slot, z, x, 1)
        add_pairs(
            [(1, [12 * (p // 2) + 3 * (p % 2)], [(p, 2)], False) for p in range(4)]
        )
        update(slot)
        for copy in copies:
            copy.wait_send()
        return carry

    constant_parts()
    pl.semaphore_wait(barrier, expected)

    @pl.when(jnp.logical_not(at_home))
    def _():
        delivery.start()
        delivery.wait_recv()
        delivery.wait_send()

    @pl.when(at_home)
    def _():
        hosted[...] = parcel[...]

    unpack()
    lax.fori_loop(0, STEPS, one_step, 0)

    states, moves = [], []
    for cell in range(8):
        z, x, y = cell // 4, cell // 2 % 2, cell % 2
        here = region[STEPS, 1 + z, 1 + x, y]
        moved = jnp.concatenate([here, speed[cell // 2, 4 * y : 4 * y + 4]], axis=0)
        live = jnp.broadcast_to(here[3:4], (8, ATOMS)) > 0.0
        states.append(jnp.where(live & is_xyz, moved, 0.0))
    for r in range(8):
        y = shift_y(me_y, r)
        base = (((me_z * n_x + me_x) * n_y + y) * SEATS).astype(F32)
        message = jnp.where(row8 == 3, -1.0, 0.0)
        for cell in range(8):
            seat = seat_ref[cell] - base
            hit = (seat >= 0.0) & (seat < float(SEATS))
            tagged = jnp.where(row8 == 3, seat, states[cell])
            if r == 0:
                stay_send[cell] = jnp.where(hit, tagged, jnp.where(row8 == 3, -1.0, 0.0))
            else:
                message = jnp.where(hit, tagged, message)
        if r > 0:
            send_box[r - 1] = message
        src, dst = (stay_send, stay_box) if r == 0 else (send_box.at[r - 1], box.at[r - 1])
        move = pltpu.make_async_remote_copy(
            src_ref=src,
            dst_ref=dst,
            send_sem=move_send_sem.at[r],
            recv_sem=move_recv_sem.at[r],
            device_id=(me_z, me_x, y),
            device_id_type=MESH,
        )
        moves.append(move)

        @pl.when(jnp.logical_not(goes_to_itself(r)))
        def _():
            move.start()

        @pl.when(goes_to_itself(r))
        def _():
            dst[...] = src[...]

    for r in range(8):

        @pl.when(jnp.logical_not(goes_to_itself(r)))
        def _():
            moves[r].wait_recv()

    messages = [stay_box[cell] for cell in range(8)] + [box[r] for r in range(7)]
    marks = [jnp.broadcast_to(m[3:4], (8, ATOMS)) for m in messages]
    for seat in range(SEATS):
        result = zero8
        for mark, message in zip(marks, messages):
            result = jnp.where(mark == float(seat), message, result)
        for k in range(3):
            out_pos_ref[k, pl.ds(seat, 1), :] = result[k : k + 1]
            out_vel_ref[k, pl.ds(seat, 1), :] = result[4 + k : 5 + k]
    for r in range(8):

        @pl.when(jnp.logical_not(goes_to_itself(r)))
        def _():
            moves[r].wait_send()


def on_device(positions, velocities, types, strength, counts, pair_list, destination):
    vmem = pl.BlockSpec(memory_space=pltpu.VMEM)
    smem = pl.BlockSpec(memory_space=pltpu.SMEM)
    shape = jax.ShapeDtypeStruct((3, SEATS, ATOMS), F32)
    return pl.pallas_call(
        body,
        out_shape=(shape, shape),
        in_specs=[vmem, vmem, vmem, smem, smem, vmem, smem],
        out_specs=(vmem, vmem),
        scratch_shapes=[
            pltpu.VMEM((STEPS + 1, 4, 4, 4, 4, ATOMS), F32),
            pltpu.VMEM((4, 8, ATOMS), F32),
            pltpu.VMEM((8, 8, ATOMS), F32),
            pltpu.VMEM((9, 8, ATOMS), F32),
            pltpu.VMEM((9, 8, ATOMS), F32),
            pltpu.VMEM((8, 32, ATOMS), F32),
            pltpu.VMEM((2, 16, ATOMS, DEPTH), BF16),
            pltpu.VMEM((4, DEPTH, 6 * ATOMS), BF16),
            pltpu.VMEM((2, 16, 16 * ATOMS), BF16),
            pltpu.VMEM((4, 3, 16, 2 * ATOMS), F32),
            pltpu.VMEM((7, 8, ATOMS), F32),
            pltpu.VMEM((8, 8, ATOMS), F32),
            pltpu.VMEM((7, 8, ATOMS), F32),
            pltpu.VMEM((8, 8, ATOMS), F32),
            pltpu.SemaphoreType.DMA((STEPS, 26)),
            pltpu.SemaphoreType.DMA((STEPS, 26)),
            pltpu.SemaphoreType.DMA((2,)),
            pltpu.SemaphoreType.DMA((8,)),
            pltpu.SemaphoreType.DMA((8,)),
        ],
        compiler_params=pltpu.CompilerParams(collective_id=0, has_side_effects=True),
    )(positions, velocities, types, strength, counts, pair_list.transpose(1, 2, 3, 0), destination)


def solution(mesh):
    return jax.shard_map(
        on_device,
        mesh=mesh,
        in_specs=(
            P(None, "tower", "px", "py", None),
            P(None, "tower", "px", "py", None),
            P("tower", "px", "py", None),
            P(),
            P("tower", "px", "py"),
            P(None, "tower", "px", "py"),
            P("tower", "px", "py"),
        ),
        out_specs=(P(None, ("tower", "px", "py"), None), P(None, ("tower", "px", "py"), None)),
        check_vma=False,
    )
```

```python
import itertools

import jax
import jax.numpy as jnp
from jax import lax
from jax.experimental import pallas as pl
from jax.experimental.pallas import tpu as pltpu
from jax.sharding import PartitionSpec as P

STEPS = 4
STEP_TIME = 0.02
KINDS = 16
SEATS = 15
ATOMS = 128
DEPTH = 112
CHUNK, AHEAD = 2, 2
MESH = pl.DeviceIdType.MESH
F32 = jnp.float32
BF16 = jnp.bfloat16

DIRECTIONS = sorted(
    (d for d in itertools.product((-1, 0, 1), repeat=3) if d != (0, 0, 0)),
    key=lambda d: (sum(map(abs, d)), abs(d[1]) + abs(d[2])),
)
NEAREST, FACES, EDGES = 2, 6, 18
SEAT_OF_Y = {0: 0, 1: 1, -1: 2, 2: 3}


def spans(step):
    if step == 0:
        return pl.ds(1, 2), pl.ds(1, 2)
    return (pl.ds(2, 1), pl.ds(0, 1)) if step == 1 else (pl.ds(1, 1), pl.ds(3, 1))


def spans_y(step):
    if step == 0:
        return pl.ds(0, 2), pl.ds(0, 2)
    return (pl.ds(1, 1), pl.ds(2, 1)) if step == 1 else (pl.ds(0, 1), pl.ds(3, 1))


def thirds(x):
    high = x.astype(BF16).astype(F32)
    rest = x - high
    mid = rest.astype(BF16).astype(F32)
    return high, mid, rest - mid


def swap_halves(x):
    return jnp.concatenate([x[4:], x[:4]], axis=0)


def host_of(t, x, y):
    return (2 * (t // 2) + y // 4, x, 2 * lax.rem(y, 4) + lax.rem(t, 2))


def body(*refs):
    inputs, (out_pos_ref, out_vel_ref), local = refs[:7], refs[7:9], refs[9:16]
    program(inputs, local, out_pos_ref, out_vel_ref, *refs[16:])


def program(
    inputs, local, out_pos_ref, out_vel_ref, load_sem,
    region, speed, seat_ref, parcel, hosted, flag_ref, left_ref, right_ref, value_ref, total,
    box, stay_box, send_box, stay_send,
    send_sem, recv_sem, host_sem, move_send_sem, move_recv_sem,
):
    pos_ref, vel_ref, types_ref, strength_ref, counts_ref, pair_ref, dest_ref = local
    loads = [
        pltpu.make_async_copy(source, target, load_sem.at[i])
        for i, (source, target) in enumerate(zip(inputs, local))
    ]
    for load in loads:
        load.start()
    home_t, home_x, home_y = (lax.axis_index(a) for a in ("tower", "px", "py"))
    n_z, n_x, n_y = (lax.axis_size(a) for a in ("tower", "px", "py"))
    me_z = 2 * (home_t // 2) + lax.rem(home_y, 2)
    me_x = home_x
    me_y = 4 * lax.rem(home_t, 2) + home_y // 2
    host = host_of(home_t, home_x, home_y)
    same_tower = me_z == home_t
    at_home = jnp.logical_and(same_tower, me_y == home_y)

    def device(d):
        return host_of(
            lax.rem(me_z + d[0] + n_z, n_z),
            lax.rem(me_x + d[1] + n_x, n_x),
            lax.rem(me_y + d[2] + n_y, n_y),
        )

    def shift_y(y, r):
        return lax.rem(y + r + n_y, n_y)

    def goes_to_itself(r):
        return jnp.logical_and(same_tower, shift_y(me_y, r) == home_y)

    barrier = pltpu.get_barrier_semaphore()

    def greet(target):
        pl.semaphore_signal(barrier, inc=1, device_id=target, device_id_type=MESH)

    @pl.when(jnp.logical_not(at_home))
    def _():
        greet((me_z, me_x, me_y))

    for d in DIRECTIONS:
        greet(device(d))
    for r in range(8):

        @pl.when(jnp.logical_not(goes_to_itself(r)))
        def _():
            greet(host_of(home_t, home_x, shift_y(home_y, -r)))

    expected = len(DIRECTIONS) + 9 - at_home.astype(jnp.int32) - same_tower.astype(jnp.int32)

    row8 = lax.broadcasted_iota(jnp.int32, (8, ATOMS), 0)
    row16 = lax.broadcasted_iota(jnp.int32, (16, ATOMS), 0)
    low = row8 < 4
    comp = lax.rem(row8, 4)
    is_xyz = comp < 3
    zero8 = jnp.zeros((8, ATOMS), F32)

    for load in loads:
        load.wait()

    kinds = types_ref[...].reshape(8, ATOMS)
    table = jnp.zeros((8, ATOMS), F32)
    for kind in range(KINDS):
        table = jnp.where(kinds == kind, strength_ref[kind], table)
    lanes = lax.broadcasted_iota(jnp.int32, (1, ATOMS), 1)
    parcel[8] = zero8
    for cell in range(8):
        z, x, y = cell // 4, cell // 2 % 2, cell % 2
        live = (lanes < counts_ref[z, x, y]).astype(F32)
        for k in range(3):
            parcel[cell, pl.ds(k, 1), :] = pos_ref[k, z, x, pl.ds(y, 1), :]
            parcel[cell, pl.ds(4 + k, 1), :] = vel_ref[k, z, x, pl.ds(y, 1), :]
        parcel[cell, pl.ds(3, 1), :] = table[cell : cell + 1] * live
        seat = dest_ref[z, x, y].astype(F32)
        parcel[cell, pl.ds(7, 1), :] = jnp.full((1, ATOMS), seat, F32)
        parcel[8, pl.ds(cell, 1), pl.ds(0, 27)] = pair_ref[z, x, pl.ds(y, 1), :].astype(F32)
    delivery = pltpu.make_async_remote_copy(
        src_ref=parcel,
        dst_ref=hosted,
        send_sem=host_sem.at[0],
        recv_sem=host_sem.at[1],
        device_id=host,
        device_id_type=MESH,
    )

    def halo_copies(slot):
        copies = []
        for i, d in enumerate(DIRECTIONS):
            (sz, tz), (sx, tx), (sy, ty) = spans(d[0]), spans(d[1]), spans_y(d[2])
            copies.append(
                pltpu.make_async_remote_copy(
                    src_ref=region.at[slot, sz, sx, sy],
                    dst_ref=region.at[slot, tz, tx, ty],
                    send_sem=send_sem.at[slot, i],
                    recv_sem=recv_sem.at[slot, i],
                    device_id=device(d),
                    device_id_type=MESH,
                )
            )
        return copies

    def constant_parts():
        for p in range(4):
            for t in range(3):
                for side in range(2):
                    half = ((0, 0), (1, 1), (0, 1))[t][side]
                    mark = jnp.where((low if half == 0 else ~low) & is_xyz, -1.0, 0.0)
                    right_ref[p, 80:96, pl.ds(256 * t + 128 * side, 128)] = jnp.concatenate(
                        [mark, mark], axis=0
                    ).astype(BF16)

    def unpack():
        for cell in range(8):
            z, x, y = cell // 4, cell // 2 % 2, cell % 2
            tile = hosted[cell]
            region[0, 1 + z, 1 + x, y] = tile[:4]
            speed[cell // 2, pl.ds(4 * y, 4), :] = jnp.where(row8[:4] < 3, tile[4:], 0.0)
            seat_ref[cell] = jnp.broadcast_to(tile[7:8], (8, ATOMS))
        padded = jnp.concatenate([(hosted[8] - 1.0) * 100.0] + [zero8] * 15, axis=0)
        turned = padded.T
        for cell in range(8):
            flag_ref[cell] = jnp.broadcast_to(turned[:32, cell : cell + 1], (32, ATOMS))
        for p, side in itertools.product(range(4), range(2)):
            cell, z, x = 2 * p + side, p // 2, p % 2
            rows32 = flag_ref[cell]
            for t in range(3):
                y = ((0, 0), (1, 1), (-1, 2))[t][side] - side + 1
                rows = [jnp.zeros((1, ATOMS), F32)] * 16
                for oz, ox in itertools.product(range(3), range(3)):
                    k = 9 * oz + 3 * ox + y
                    rows[4 * (z + oz) + x + ox] = rows32[k : k + 1]
                right_ref[p, 96:112, pl.ds(256 * t + 128 * side, 128)] = jnp.concatenate(
                    rows, axis=0
                ).astype(BF16)

    def shift_of(z, x, part):
        y_low, y_high = ((-1.0, 0.0), (-2.0, 1.0))[part]
        y = jnp.where(low, y_low, y_high)
        return jnp.where(
            comp == 0, z - 2.0, jnp.where(comp == 1, x - 2.0, jnp.where(comp == 2, y, 0.0))
        )

    def own_tile(slot, z, x, part):
        return jnp.concatenate(
            [region[slot, z, x, 2 * part], region[slot, z, x, 2 * part + 1]], axis=0
        )

    def strength_rows(tile):
        return jnp.concatenate(
            [
                jnp.broadcast_to(tile[3:4], (4, ATOMS)),
                jnp.broadcast_to(tile[7:8], (4, ATOMS)),
            ],
            axis=0,
        )

    def build_left(slot, z, x, part):
        column = 4 * z + x
        raw = own_tile(slot, z, x, part)
        tile = raw + shift_of(z, x, part)
        high, mid, rest = thirds(tile)
        ones = jnp.ones((24, ATOMS), F32)
        rows = [high, high, mid, mid, high, rest, ones, *thirds(tile * tile)]
        rows += [jnp.where(row16 == column, 1.0, 0.0)]
        left_ref[part, column] = jnp.concatenate(rows, axis=0).astype(BF16).T
        value = jnp.where(is_xyz, tile, 1.0) * strength_rows(raw)
        high = value.astype(BF16).astype(F32)
        value_ref[part, :, pl.ds(128 * column, 128)] = jnp.concatenate(
            [high, value - high], axis=0
        ).astype(BF16)

    def build_right(slot):
        for p in range(4):
            z, x = 1 + p // 2, 1 + p % 2
            tile = own_tile(slot, z, x, 0) + shift_of(z, x, 0)
            tile = jnp.where(is_xyz, tile, 0.0)
            terms = [2.0 * v for v in thirds(tile)]
            swapped = [swap_halves(v) for v in terms]
            squares = [-v for v in thirds(tile * tile)]
            squares[0] = jnp.where(is_xyz, squares[0], 1.0)
            for side in range(2):
                mine = low if side == 0 else ~low
                norms = [jnp.where(mine, v, 0.0) for v in squares]
                for t in range(3):
                    half = ((0, 0), (1, 1), (0, 1))[t][side]
                    keep = low if half == 0 else ~low
                    source = terms if half == side else swapped
                    high, mid, rest = [jnp.where(keep, v, 0.0) for v in source]
                    mark = jnp.where(keep & is_xyz, -1.0, 0.0)
                    rows = [high, mid, high, mid, rest, high, *norms, mark]
                    right_ref[p, 0:80, pl.ds(256 * t + 128 * side, 128)] = jnp.concatenate(
                        rows, axis=0
                    ).astype(BF16)

    def nearness(part, columns, targets):
        lhs = jnp.concatenate([left_ref[part, c] for c in columns], axis=0)
        rhs = jnp.concatenate(
            [right_ref[p, :, pl.ds(256 * t, 256)] for p, t in targets], axis=1
        )
        return jnp.dot(lhs, rhs, preferred_element_type=F32)

    def add_sums(near, part, columns, targets, first):
        near = jnp.maximum(near, 0.0)
        weight = near * near
        high = weight.astype(BF16)
        rest = (weight - high.astype(F32)).astype(BF16)
        values = jnp.concatenate(
            [value_ref[part, :, pl.ds(128 * c, 128)] for c in columns], axis=1
        )
        add = jnp.dot(values, high, preferred_element_type=F32) + jnp.dot(
            values, rest, preferred_element_type=F32
        )
        for i, (p, t) in enumerate(targets):
            more = add[:, 256 * i : 256 * i + 256]
            if first:
                total[p, t] = more
            else:
                total[p, t] += more

    def add_pairs(groups):
        parts = [
            (part, columns[at : at + CHUNK], targets, first and at == 0)
            for part, columns, targets, first in groups
            for at in range(0, len(columns), CHUNK)
        ]
        waiting = []
        for group in parts:
            waiting.append((nearness(*group[:3]), *group))
            if len(waiting) > AHEAD:
                add_sums(*waiting.pop(0))
        for group in waiting:
            add_sums(*group)

    def update(slot):
        for p in range(4):
            z, x = 1 + p // 2, 1 + p % 2
            both = total[p, 0]
            both = both[:8] + both[8:]
            other = total[p, 1]
            other = other[:8] + other[8:]
            apart = total[p, 2]
            apart = apart[:8] + apart[8:]
            sums = jnp.concatenate(
                [
                    both[:4, :128] + other[4:, :128] + apart[:4, :128],
                    both[:4, 128:] + other[4:, 128:] + apart[4:, 128:],
                ],
                axis=0,
            )
            raw = own_tile(slot, z, x, 0)
            tile = raw + shift_of(z, x, 0)
            force = -6.0 * strength_rows(raw) * (sums - tile * strength_rows(sums))
            new_speed = speed[p] + STEP_TIME * jnp.where(is_xyz, force, 0.0)
            speed[p] = new_speed
            new = raw + STEP_TIME * new_speed
            region[slot + 1, z, x, 0] = new[:4]
            region[slot + 1, z, x, 1] = new[4:]

    inner = (1, 2)
    own = [(z, x) for z in inner for x in inner]
    beside = [(z, x) for z in (0, 3) for x in inner] + [(z, x) for z in inner for x in (0, 3)]
    across = [(z, x) for z in (0, 3) for x in (0, 3)]

    def one_step(slot, carry):
        copies = halo_copies(slot)
        for copy in copies:
            copy.start()
        build_right(slot)
        for z, x in own:
            build_left(slot, z, x, 0)
        add_pairs([(0, [5, 6, 9, 10], [(p, 0), (p, 1)], True) for p in range(4)])
        for copy in copies[:NEAREST]:
            copy.wait_recv()
        for z in (0, 3):
            for x in inner:
                build_left(slot, z, x, 0)
        add_pairs(
            [
                (0, [12 * (p // 2) + 1, 12 * (p // 2) + 2], [(p, 0), (p, 1)], False)
                for p in range(4)
            ]
        )
        for copy in copies[NEAREST:FACES]:
            copy.wait_recv()
        for z, x in own:
            build_left(slot, z, x, 1)
        for z in inner:
            for x in (0, 3):
                build_left(slot, z, x, 0)
        add_pairs(
            [(1, [5, 6, 9, 10], [(p, 2), (p + 1, 2)], True) for p in (0, 2)]
            + [
                (0, [4 + 3 * (p % 2), 8 + 3 * (p % 2)], [(p, 0), (p, 1)], False)
                for p in range(4)
            ]
        )
        for copy in copies[FACES:EDGES]:
            copy.wait_recv()
        for z, x in beside:
            build_left(slot, z, x, 1)
        for z, x in across:
            build_left(slot, z, x, 0)
        add_pairs(
            [(1, [12 * i + 1, 12 * i + 2], [(2 * i, 2), (2 * i + 1, 2)], False) for i in (0, 1)]
            + [(1, [4 + 3 * i, 8 + 3 * i], [(i, 2), (2 + i, 2)], False) for i in (0, 1)]
            + [
                (0, [12 * (p // 2) + 3 * (p % 2)], [(p, 0), (p, 1)], False)
                for p in range(4)
            ]
        )
        for copy in copies[EDGES:]:
            copy.wait_recv()
        for z, x in across:
            build_left(slot, z, x, 1)
        add_pairs(
            [(1, [12 * (p // 2) + 3 * (p % 2)], [(p, 2)], False) for p in range(4)]
        )
        update(slot)
        for copy in copies:
            copy.wait_send()
        return carry

    constant_parts()
    pl.semaphore_wait(barrier, expected)

    @pl.when(jnp.logical_not(at_home))
    def _():
        delivery.start()
        delivery.wait_recv()
        delivery.wait_send()

    @pl.when(at_home)
    def _():
        hosted[...] = parcel[...]

    unpack()
    lax.fori_loop(0, STEPS, one_step, 0)

    states, moves = [], []
    for cell in range(8):
        z, x, y = cell // 4, cell // 2 % 2, cell % 2
        here = region[STEPS, 1 + z, 1 + x, y]
        moved = jnp.concatenate([here, speed[cell // 2, 4 * y : 4 * y + 4]], axis=0)
        live = jnp.broadcast_to(here[3:4], (8, ATOMS)) > 0.0
        states.append(jnp.where(live & is_xyz, moved, 0.0))
    for r in range(8):
        y = shift_y(me_y, r)
        base = (((me_z * n_x + me_x) * n_y + y) * SEATS).astype(F32)
        message = jnp.where(row8 == 3, -1.0, 0.0)
        for cell in range(8):
            seat = seat_ref[cell] - base
            hit = (seat >= 0.0) & (seat < float(SEATS))
            tagged = jnp.where(row8 == 3, seat, states[cell])
            if r == 0:
                stay_send[cell] = jnp.where(hit, tagged, jnp.where(row8 == 3, -1.0, 0.0))
            else:
                message = jnp.where(hit, tagged, message)
        if r > 0:
            send_box[r - 1] = message
        src, dst = (stay_send, stay_box) if r == 0 else (send_box.at[r - 1], box.at[r - 1])
        move = pltpu.make_async_remote_copy(
            src_ref=src,
            dst_ref=dst,
            send_sem=move_send_sem.at[r],
            recv_sem=move_recv_sem.at[r],
            device_id=(me_z, me_x, y),
            device_id_type=MESH,
        )
        moves.append(move)

        @pl.when(jnp.logical_not(goes_to_itself(r)))
        def _():
            move.start()

        @pl.when(goes_to_itself(r))
        def _():
            dst[...] = src[...]

    for r in range(8):

        @pl.when(jnp.logical_not(goes_to_itself(r)))
        def _():
            moves[r].wait_recv()

    messages = [stay_box[cell] for cell in range(8)] + [box[r] for r in range(7)]
    marks = [jnp.broadcast_to(m[3:4], (8, ATOMS)) for m in messages]
    for seat in range(SEATS):
        result = zero8
        for mark, message in zip(marks, messages):
            result = jnp.where(mark == float(seat), message, result)
        for k in range(3):
            out_pos_ref[k, pl.ds(seat, 1), :] = result[k : k + 1]
            out_vel_ref[k, pl.ds(seat, 1), :] = result[4 + k : 5 + k]
    for r in range(8):

        @pl.when(jnp.logical_not(goes_to_itself(r)))
        def _():
            moves[r].wait_send()


def on_device(positions, velocities, types, strength, counts, pair_list, destination):
    vmem = pl.BlockSpec(memory_space=pltpu.VMEM)
    shape = pltpu.VMEM((3, SEATS, ATOMS), F32)
    return pl.pallas_call(
        body,
        out_shape=(shape, shape),
        in_specs=[pl.BlockSpec(memory_space=pl.ANY)] * 7,
        out_specs=(vmem, vmem),
        scratch_shapes=[
            pltpu.VMEM((3, 2, 2, 2, ATOMS), F32),
            pltpu.VMEM((3, 2, 2, 2, ATOMS), F32),
            pltpu.VMEM((2, 2, 2, ATOMS), jnp.int32),
            pltpu.SMEM((KINDS,), F32),
            pltpu.SMEM((2, 2, 2), jnp.int32),
            pltpu.VMEM((2, 2, 2, 27), jnp.int32),
            pltpu.SMEM((2, 2, 2), jnp.int32),
            pltpu.SemaphoreType.DMA((7,)),
            pltpu.VMEM((STEPS + 1, 4, 4, 4, 4, ATOMS), F32),
            pltpu.VMEM((4, 8, ATOMS), F32),
            pltpu.VMEM((8, 8, ATOMS), F32),
            pltpu.VMEM((9, 8, ATOMS), F32),
            pltpu.VMEM((9, 8, ATOMS), F32),
            pltpu.VMEM((8, 32, ATOMS), F32),
            pltpu.VMEM((2, 16, ATOMS, DEPTH), BF16),
            pltpu.VMEM((4, DEPTH, 6 * ATOMS), BF16),
            pltpu.VMEM((2, 16, 16 * ATOMS), BF16),
            pltpu.VMEM((4, 3, 16, 2 * ATOMS), F32),
            pltpu.VMEM((7, 8, ATOMS), F32),
            pltpu.VMEM((8, 8, ATOMS), F32),
            pltpu.VMEM((7, 8, ATOMS), F32),
            pltpu.VMEM((8, 8, ATOMS), F32),
            pltpu.SemaphoreType.DMA((STEPS, 26)),
            pltpu.SemaphoreType.DMA((STEPS, 26)),
            pltpu.SemaphoreType.DMA((2,)),
            pltpu.SemaphoreType.DMA((8,)),
            pltpu.SemaphoreType.DMA((8,)),
        ],
        compiler_params=pltpu.CompilerParams(collective_id=0, has_side_effects=True),
    )(positions, velocities, types, strength, counts, pair_list.transpose(1, 2, 3, 0), destination)


def solution(mesh):
    return jax.shard_map(
        on_device,
        mesh=mesh,
        in_specs=(
            P(None, "tower", "px", "py", None),
            P(None, "tower", "px", "py", None),
            P("tower", "px", "py", None),
            P(),
            P("tower", "px", "py"),
            P(None, "tower", "px", "py"),
            P("tower", "px", "py"),
        ),
        out_specs=(P(None, ("tower", "px", "py"), None), P(None, ("tower", "px", "py"), None)),
        check_vma=False,
    )
```

```python
import itertools

import jax
import jax.numpy as jnp
from jax import lax
from jax.experimental import pallas as pl
from jax.experimental.pallas import tpu as pltpu
from jax.sharding import PartitionSpec as P

STEPS = 4
STEP_TIME = 0.02
KINDS = 16
SEATS = 15
ATOMS = 128
DEPTH = 112
CHUNK, AHEAD = 2, 2
MESH = pl.DeviceIdType.MESH
F32 = jnp.float32
BF16 = jnp.bfloat16

DIRECTIONS = sorted(
    (d for d in itertools.product((-1, 0, 1), repeat=3) if d != (0, 0, 0)),
    key=lambda d: (sum(map(abs, d)), abs(d[1]) + abs(d[2])),
)
NEAREST, FACES, EDGES = 2, 6, 18
SEAT_OF_Y = {0: 0, 1: 1, -1: 2, 2: 3}


def spans(step):
    if step == 0:
        return pl.ds(1, 2), pl.ds(1, 2)
    return (pl.ds(2, 1), pl.ds(0, 1)) if step == 1 else (pl.ds(1, 1), pl.ds(3, 1))


def spans_y(step):
    if step == 0:
        return pl.ds(0, 2), pl.ds(0, 2)
    return (pl.ds(1, 1), pl.ds(2, 1)) if step == 1 else (pl.ds(0, 1), pl.ds(3, 1))


def thirds(x):
    high = x.astype(BF16).astype(F32)
    rest = x - high
    mid = rest.astype(BF16).astype(F32)
    return high, mid, rest - mid


def swap_halves(x):
    return jnp.concatenate([x[4:], x[:4]], axis=0)


def host_of(t, x, y):
    return (2 * (t // 2) + y // 4, x, 2 * lax.rem(y, 4) + lax.rem(t, 2))


def body(*refs):
    inputs, (out_pos_ref, out_vel_ref), local = refs[:7], refs[7:9], refs[9:16]
    program(inputs, local, out_pos_ref, out_vel_ref, *refs[16:])


def program(
    inputs, local, out_pos_ref, out_vel_ref, load_sem,
    region, speed, seat_ref, parcel, hosted, flag_ref, left_ref, right_ref, value_ref, total,
    box, stay_box, send_box, stay_send,
    send_sem, recv_sem, host_sem, move_send_sem, move_recv_sem,
):
    pos_ref, vel_ref, types_ref, strength_ref, counts_ref, pair_ref, dest_ref = local
    loads = [
        pltpu.make_async_copy(source, target, load_sem.at[i])
        for i, (source, target) in enumerate(zip(inputs, local))
    ]
    for load in loads:
        load.start()
    home_t, home_x, home_y = (lax.axis_index(a) for a in ("tower", "px", "py"))
    n_z, n_x, n_y = (lax.axis_size(a) for a in ("tower", "px", "py"))
    me_z = 2 * (home_t // 2) + lax.rem(home_y, 2)
    me_x = home_x
    me_y = 4 * lax.rem(home_t, 2) + home_y // 2
    host = host_of(home_t, home_x, home_y)
    same_tower = me_z == home_t
    at_home = jnp.logical_and(same_tower, me_y == home_y)

    def device(d):
        return host_of(
            lax.rem(me_z + d[0] + n_z, n_z),
            lax.rem(me_x + d[1] + n_x, n_x),
            lax.rem(me_y + d[2] + n_y, n_y),
        )

    def shift_y(y, r):
        return lax.rem(y + r + n_y, n_y)

    def goes_to_itself(r):
        return jnp.logical_and(same_tower, shift_y(me_y, r) == home_y)

    barrier = pltpu.get_barrier_semaphore()

    def greet(target):
        pl.semaphore_signal(barrier, inc=1, device_id=target, device_id_type=MESH)

    @pl.when(jnp.logical_not(at_home))
    def _():
        greet((me_z, me_x, me_y))

    targets = [device(d) for d in DIRECTIONS]
    for target in targets:
        greet(target)
    for r in range(8):

        @pl.when(jnp.logical_not(goes_to_itself(r)))
        def _():
            greet(host_of(home_t, home_x, shift_y(home_y, -r)))

    expected = len(DIRECTIONS) + 9 - at_home.astype(jnp.int32) - same_tower.astype(jnp.int32)

    row8 = lax.broadcasted_iota(jnp.int32, (8, ATOMS), 0)
    row16 = lax.broadcasted_iota(jnp.int32, (16, ATOMS), 0)
    low = row8 < 4
    comp = lax.rem(row8, 4)
    is_xyz = comp < 3
    zero8 = jnp.zeros((8, ATOMS), F32)

    for load in loads:
        load.wait()

    kinds = types_ref[...].reshape(8, ATOMS)
    table = jnp.zeros((8, ATOMS), F32)
    for kind in range(KINDS):
        table = jnp.where(kinds == kind, strength_ref[kind], table)
    lanes = lax.broadcasted_iota(jnp.int32, (1, ATOMS), 1)
    parcel[8] = zero8
    for cell in range(8):
        z, x, y = cell // 4, cell // 2 % 2, cell % 2
        live = (lanes < counts_ref[z, x, y]).astype(F32)
        for k in range(3):
            parcel[cell, pl.ds(k, 1), :] = pos_ref[k, z, x, pl.ds(y, 1), :]
            parcel[cell, pl.ds(4 + k, 1), :] = vel_ref[k, z, x, pl.ds(y, 1), :]
        parcel[cell, pl.ds(3, 1), :] = table[cell : cell + 1] * live
        seat = dest_ref[z, x, y].astype(F32)
        parcel[cell, pl.ds(7, 1), :] = jnp.full((1, ATOMS), seat, F32)
        parcel[8, pl.ds(cell, 1), pl.ds(0, 27)] = pair_ref[z, x, pl.ds(y, 1), :].astype(F32)
    delivery = pltpu.make_async_remote_copy(
        src_ref=parcel,
        dst_ref=hosted,
        send_sem=host_sem.at[0],
        recv_sem=host_sem.at[1],
        device_id=host,
        device_id_type=MESH,
    )

    def halo_copies(slot):
        copies = []
        for i, d in enumerate(DIRECTIONS):
            (sz, tz), (sx, tx), (sy, ty) = spans(d[0]), spans(d[1]), spans_y(d[2])
            copies.append(
                pltpu.make_async_remote_copy(
                    src_ref=region.at[slot, sz, sx, sy],
                    dst_ref=region.at[slot, tz, tx, ty],
                    send_sem=send_sem.at[slot, i],
                    recv_sem=recv_sem.at[slot, i],
                    device_id=targets[i],
                    device_id_type=MESH,
                )
            )
        return copies

    def constant_parts():
        for p in range(4):
            for t in range(3):
                for side in range(2):
                    half = ((0, 0), (1, 1), (0, 1))[t][side]
                    mark = jnp.where((low if half == 0 else ~low) & is_xyz, -1.0, 0.0)
                    right_ref[p, 80:96, pl.ds(256 * t + 128 * side, 128)] = jnp.concatenate(
                        [mark, mark], axis=0
                    ).astype(BF16)

    def unpack():
        for cell in range(8):
            z, x, y = cell // 4, cell // 2 % 2, cell % 2
            tile = hosted[cell]
            region[0, 1 + z, 1 + x, y] = tile[:4]
            speed[cell // 2, pl.ds(4 * y, 4), :] = jnp.where(row8[:4] < 3, tile[4:], 0.0)
            seat_ref[cell] = jnp.broadcast_to(tile[7:8], (8, ATOMS))
        padded = jnp.concatenate([(hosted[8] - 1.0) * 100.0] + [zero8] * 15, axis=0)
        turned = padded.T
        for cell in range(8):
            flag_ref[cell] = jnp.broadcast_to(turned[:32, cell : cell + 1], (32, ATOMS))
        for p, side in itertools.product(range(4), range(2)):
            cell, z, x = 2 * p + side, p // 2, p % 2
            rows32 = flag_ref[cell]
            for t in range(3):
                y = ((0, 0), (1, 1), (-1, 2))[t][side] - side + 1
                rows = [jnp.zeros((1, ATOMS), F32)] * 16
                for oz, ox in itertools.product(range(3), range(3)):
                    k = 9 * oz + 3 * ox + y
                    rows[4 * (z + oz) + x + ox] = rows32[k : k + 1]
                right_ref[p, 96:112, pl.ds(256 * t + 128 * side, 128)] = jnp.concatenate(
                    rows, axis=0
                ).astype(BF16)

    def shift_of(z, x, part):
        y_low, y_high = ((-1.0, 0.0), (-2.0, 1.0))[part]
        y = jnp.where(low, y_low, y_high)
        return jnp.where(
            comp == 0, z - 2.0, jnp.where(comp == 1, x - 2.0, jnp.where(comp == 2, y, 0.0))
        )

    def own_tile(slot, z, x, part):
        return jnp.concatenate(
            [region[slot, z, x, 2 * part], region[slot, z, x, 2 * part + 1]], axis=0
        )

    def strength_rows(tile):
        return jnp.concatenate(
            [
                jnp.broadcast_to(tile[3:4], (4, ATOMS)),
                jnp.broadcast_to(tile[7:8], (4, ATOMS)),
            ],
            axis=0,
        )

    def build_left(slot, z, x, part):
        column = 4 * z + x
        raw = own_tile(slot, z, x, part)
        tile = raw + shift_of(z, x, part)
        high, mid, rest = thirds(tile)
        ones = jnp.ones((24, ATOMS), F32)
        rows = [high, high, mid, mid, high, rest, ones, *thirds(tile * tile)]
        rows += [jnp.where(row16 == column, 1.0, 0.0)]
        left_ref[part, column] = jnp.concatenate(rows, axis=0).astype(BF16).T
        value = jnp.where(is_xyz, tile, 1.0) * strength_rows(raw)
        high = value.astype(BF16).astype(F32)
        value_ref[part, :, pl.ds(128 * column, 128)] = jnp.concatenate(
            [high, value - high], axis=0
        ).astype(BF16)

    def build_right(slot):
        for p in range(4):
            z, x = 1 + p // 2, 1 + p % 2
            tile = own_tile(slot, z, x, 0) + shift_of(z, x, 0)
            tile = jnp.where(is_xyz, tile, 0.0)
            terms = [2.0 * v for v in thirds(tile)]
            swapped = [swap_halves(v) for v in terms]
            squares = [-v for v in thirds(tile * tile)]
            squares[0] = jnp.where(is_xyz, squares[0], 1.0)
            for side in range(2):
                mine = low if side == 0 else ~low
                norms = [jnp.where(mine, v, 0.0) for v in squares]
                for t in range(3):
                    half = ((0, 0), (1, 1), (0, 1))[t][side]
                    keep = low if half == 0 else ~low
                    source = terms if half == side else swapped
                    high, mid, rest = [jnp.where(keep, v, 0.0) for v in source]
                    mark = jnp.where(keep & is_xyz, -1.0, 0.0)
                    rows = [high, mid, high, mid, rest, high, *norms, mark]
                    right_ref[p, 0:80, pl.ds(256 * t + 128 * side, 128)] = jnp.concatenate(
                        rows, axis=0
                    ).astype(BF16)

    def nearness(part, columns, targets):
        lhs = jnp.concatenate([left_ref[part, c] for c in columns], axis=0)
        rhs = jnp.concatenate(
            [right_ref[p, :, pl.ds(256 * t, 256)] for p, t in targets], axis=1
        )
        return jnp.dot(lhs, rhs, preferred_element_type=F32)

    def add_sums(near, part, columns, targets, first):
        near = jnp.maximum(near, 0.0)
        weight = near * near
        high = weight.astype(BF16)
        rest = (weight - high.astype(F32)).astype(BF16)
        values = jnp.concatenate(
            [value_ref[part, :, pl.ds(128 * c, 128)] for c in columns], axis=1
        )
        add = jnp.dot(values, high, preferred_element_type=F32) + jnp.dot(
            values, rest, preferred_element_type=F32
        )
        for i, (p, t) in enumerate(targets):
            more = add[:, 256 * i : 256 * i + 256]
            if first:
                total[p, t] = more
            else:
                total[p, t] += more

    def add_pairs(groups):
        parts = [
            (part, columns[at : at + CHUNK], targets, first and at == 0)
            for part, columns, targets, first in groups
            for at in range(0, len(columns), CHUNK)
        ]
        waiting = []
        for group in parts:
            waiting.append((nearness(*group[:3]), *group))
            if len(waiting) > AHEAD:
                add_sums(*waiting.pop(0))
        for group in waiting:
            add_sums(*group)

    def update(slot):
        for p in range(4):
            z, x = 1 + p // 2, 1 + p % 2
            both = total[p, 0]
            both = both[:8] + both[8:]
            other = total[p, 1]
            other = other[:8] + other[8:]
            apart = total[p, 2]
            apart = apart[:8] + apart[8:]
            sums = jnp.concatenate(
                [
                    both[:4, :128] + other[4:, :128] + apart[:4, :128],
                    both[:4, 128:] + other[4:, 128:] + apart[4:, 128:],
                ],
                axis=0,
            )
            raw = own_tile(slot, z, x, 0)
            tile = raw + shift_of(z, x, 0)
            force = -6.0 * strength_rows(raw) * (sums - tile * strength_rows(sums))
            new_speed = speed[p] + STEP_TIME * jnp.where(is_xyz, force, 0.0)
            speed[p] = new_speed
            new = raw + STEP_TIME * new_speed
            region[slot + 1, z, x, 0] = new[:4]
            region[slot + 1, z, x, 1] = new[4:]

    inner = (1, 2)
    own = [(z, x) for z in inner for x in inner]
    beside = [(z, x) for z in (0, 3) for x in inner] + [(z, x) for z in inner for x in (0, 3)]
    across = [(z, x) for z in (0, 3) for x in (0, 3)]

    def one_step(slot, carry):
        copies = halo_copies(slot)
        for copy in copies:
            copy.start()
        build_right(slot)
        for z, x in own:
            build_left(slot, z, x, 0)
        add_pairs([(0, [5, 6, 9, 10], [(p, 0), (p, 1)], True) for p in range(4)])
        for copy in copies[:NEAREST]:
            copy.wait_recv()
        for z in (0, 3):
            for x in inner:
                build_left(slot, z, x, 0)
        add_pairs(
            [
                (0, [12 * (p // 2) + 1, 12 * (p // 2) + 2], [(p, 0), (p, 1)], False)
                for p in range(4)
            ]
        )
        for copy in copies:
            copy.wait_send()
        for copy in copies[NEAREST:FACES]:
            copy.wait_recv()
        for z, x in own:
            build_left(slot, z, x, 1)
        for z in inner:
            for x in (0, 3):
                build_left(slot, z, x, 0)
        add_pairs(
            [(1, [5, 6, 9, 10], [(p, 2), (p + 1, 2)], True) for p in (0, 2)]
            + [
                (0, [4 + 3 * (p % 2), 8 + 3 * (p % 2)], [(p, 0), (p, 1)], False)
                for p in range(4)
            ]
        )
        for copy in copies[FACES:EDGES]:
            copy.wait_recv()
        for z, x in beside:
            build_left(slot, z, x, 1)
        for z, x in across:
            build_left(slot, z, x, 0)
        add_pairs(
            [(1, [12 * i + 1, 12 * i + 2], [(2 * i, 2), (2 * i + 1, 2)], False) for i in (0, 1)]
            + [(1, [4 + 3 * i, 8 + 3 * i], [(i, 2), (2 + i, 2)], False) for i in (0, 1)]
            + [
                (0, [12 * (p // 2) + 3 * (p % 2)], [(p, 0), (p, 1)], False)
                for p in range(4)
            ]
        )
        for copy in copies[EDGES:]:
            copy.wait_recv()
        for z, x in across:
            build_left(slot, z, x, 1)
        add_pairs(
            [(1, [12 * (p // 2) + 3 * (p % 2)], [(p, 2)], False) for p in range(4)]
        )
        update(slot)
        return carry

    constant_parts()
    pl.semaphore_wait(barrier, expected)

    @pl.when(jnp.logical_not(at_home))
    def _():
        delivery.start()
        delivery.wait_recv()
        delivery.wait_send()

    @pl.when(at_home)
    def _():
        hosted[...] = parcel[...]

    unpack()
    lax.fori_loop(0, STEPS, one_step, 0)

    states, moves = [], []
    for cell in range(8):
        z, x, y = cell // 4, cell // 2 % 2, cell % 2
        here = region[STEPS, 1 + z, 1 + x, y]
        moved = jnp.concatenate([here, speed[cell // 2, 4 * y : 4 * y + 4]], axis=0)
        live = jnp.broadcast_to(here[3:4], (8, ATOMS)) > 0.0
        states.append(jnp.where(live & is_xyz, moved, 0.0))
    for r in range(8):
        y = shift_y(me_y, r)
        base = (((me_z * n_x + me_x) * n_y + y) * SEATS).astype(F32)
        message = jnp.where(row8 == 3, -1.0, 0.0)
        for cell in range(8):
            seat = seat_ref[cell] - base
            hit = (seat >= 0.0) & (seat < float(SEATS))
            tagged = jnp.where(row8 == 3, seat, states[cell])
            if r == 0:
                stay_send[cell] = jnp.where(hit, tagged, jnp.where(row8 == 3, -1.0, 0.0))
            else:
                message = jnp.where(hit, tagged, message)
        if r > 0:
            send_box[r - 1] = message
        src, dst = (stay_send, stay_box) if r == 0 else (send_box.at[r - 1], box.at[r - 1])
        move = pltpu.make_async_remote_copy(
            src_ref=src,
            dst_ref=dst,
            send_sem=move_send_sem.at[r],
            recv_sem=move_recv_sem.at[r],
            device_id=(me_z, me_x, y),
            device_id_type=MESH,
        )
        moves.append(move)

        @pl.when(jnp.logical_not(goes_to_itself(r)))
        def _():
            move.start()

        @pl.when(goes_to_itself(r))
        def _():
            dst[...] = src[...]

    for r in range(8):

        @pl.when(jnp.logical_not(goes_to_itself(r)))
        def _():
            moves[r].wait_send()
            moves[r].wait_recv()

    messages = [stay_box[cell] for cell in range(8)] + [box[r] for r in range(7)]
    marks = [jnp.broadcast_to(m[3:4], (8, ATOMS)) for m in messages]
    for seat in range(SEATS):
        result = zero8
        for mark, message in zip(marks, messages):
            result = jnp.where(mark == float(seat), message, result)
        for k in range(3):
            out_pos_ref[k, pl.ds(seat, 1), :] = result[k : k + 1]
            out_vel_ref[k, pl.ds(seat, 1), :] = result[4 + k : 5 + k]


def on_device(positions, velocities, types, strength, counts, pair_list, destination):
    vmem = pl.BlockSpec(memory_space=pltpu.VMEM)
    shape = pltpu.VMEM((3, SEATS, ATOMS), F32)
    return pl.pallas_call(
        body,
        out_shape=(shape, shape),
        in_specs=[pl.BlockSpec(memory_space=pl.ANY)] * 7,
        out_specs=(vmem, vmem),
        scratch_shapes=[
            pltpu.VMEM((3, 2, 2, 2, ATOMS), F32),
            pltpu.VMEM((3, 2, 2, 2, ATOMS), F32),
            pltpu.VMEM((2, 2, 2, ATOMS), jnp.int32),
            pltpu.SMEM((KINDS,), F32),
            pltpu.SMEM((2, 2, 2), jnp.int32),
            pltpu.VMEM((2, 2, 2, 27), jnp.int32),
            pltpu.SMEM((2, 2, 2), jnp.int32),
            pltpu.SemaphoreType.DMA((7,)),
            pltpu.VMEM((STEPS + 1, 4, 4, 4, 4, ATOMS), F32),
            pltpu.VMEM((4, 8, ATOMS), F32),
            pltpu.VMEM((8, 8, ATOMS), F32),
            pltpu.VMEM((9, 8, ATOMS), F32),
            pltpu.VMEM((9, 8, ATOMS), F32),
            pltpu.VMEM((8, 32, ATOMS), F32),
            pltpu.VMEM((2, 16, ATOMS, DEPTH), BF16),
            pltpu.VMEM((4, DEPTH, 6 * ATOMS), BF16),
            pltpu.VMEM((2, 16, 16 * ATOMS), BF16),
            pltpu.VMEM((4, 3, 16, 2 * ATOMS), F32),
            pltpu.VMEM((7, 8, ATOMS), F32),
            pltpu.VMEM((8, 8, ATOMS), F32),
            pltpu.VMEM((7, 8, ATOMS), F32),
            pltpu.VMEM((8, 8, ATOMS), F32),
            pltpu.SemaphoreType.DMA((STEPS, 26)),
            pltpu.SemaphoreType.DMA((STEPS, 26)),
            pltpu.SemaphoreType.DMA((2,)),
            pltpu.SemaphoreType.DMA((8,)),
            pltpu.SemaphoreType.DMA((8,)),
        ],
        compiler_params=pltpu.CompilerParams(collective_id=0, has_side_effects=True),
    )(positions, velocities, types, strength, counts, pair_list.transpose(1, 2, 3, 0), destination)


def solution(mesh):
    return jax.shard_map(
        on_device,
        mesh=mesh,
        in_specs=(
            P(None, "tower", "px", "py", None),
            P(None, "tower", "px", "py", None),
            P("tower", "px", "py", None),
            P(),
            P("tower", "px", "py"),
            P(None, "tower", "px", "py"),
            P("tower", "px", "py"),
        ),
        out_specs=(P(None, ("tower", "px", "py"), None), P(None, ("tower", "px", "py"), None)),
        check_vma=False,
    )
```

```python
import itertools

import jax
import jax.numpy as jnp
from jax import lax
from jax.experimental import pallas as pl
from jax.experimental.pallas import tpu as pltpu
from jax.sharding import PartitionSpec as P

STEPS = 4
STEP_TIME = 0.02
KINDS = 16
SEATS = 15
ATOMS = 128
DEPTH = 112
CHUNK, AHEAD = 2, 2
MESH = pl.DeviceIdType.MESH
F32 = jnp.float32
BF16 = jnp.bfloat16

DIRECTIONS = sorted(
    (d for d in itertools.product((-1, 0, 1), repeat=3) if d != (0, 0, 0)),
    key=lambda d: (sum(map(abs, d)), abs(d[1]) + abs(d[2])),
)
NEAREST, FACES, EDGES = 2, 6, 18
SEAT_OF_Y = {0: 0, 1: 1, -1: 2, 2: 3}


def spans(step):
    if step == 0:
        return pl.ds(1, 2), pl.ds(1, 2)
    return (pl.ds(2, 1), pl.ds(0, 1)) if step == 1 else (pl.ds(1, 1), pl.ds(3, 1))


def spans_y(step):
    if step == 0:
        return pl.ds(0, 2), pl.ds(0, 2)
    return (pl.ds(1, 1), pl.ds(2, 1)) if step == 1 else (pl.ds(0, 1), pl.ds(3, 1))


def thirds(x):
    high = x.astype(BF16).astype(F32)
    rest = x - high
    mid = rest.astype(BF16).astype(F32)
    return high, mid, rest - mid


def swap_halves(x):
    return jnp.concatenate([x[4:], x[:4]], axis=0)


def host_of(t, x, y):
    return (2 * (t // 2) + y // 4, x, 2 * lax.rem(y, 4) + lax.rem(t, 2))


def body(*refs):
    inputs, (out_pos_ref, out_vel_ref), local = refs[:7], refs[7:9], refs[9:16]
    program(inputs, local, out_pos_ref, out_vel_ref, *refs[16:])


def program(
    inputs, local, out_pos_ref, out_vel_ref, load_sem,
    region, speed, seat_ref, parcel, hosted, flag_ref, left_ref, right_ref, value_ref, total,
    box, stay_box, send_box, stay_send,
    send_sem, recv_sem, host_sem, move_send_sem, move_recv_sem,
):
    pos_ref, vel_ref, types_ref, strength_ref, counts_ref, pair_ref, dest_ref = local
    loads = [
        pltpu.make_async_copy(source, target, load_sem.at[i])
        for i, (source, target) in enumerate(zip(inputs, local))
    ]
    for load in loads:
        load.start()
    home_t, home_x, home_y = (lax.axis_index(a) for a in ("tower", "px", "py"))
    n_z, n_x, n_y = (lax.axis_size(a) for a in ("tower", "px", "py"))
    me_z = 2 * (home_t // 2) + lax.rem(home_y, 2)
    me_x = home_x
    me_y = 4 * lax.rem(home_t, 2) + home_y // 2
    host = host_of(home_t, home_x, home_y)
    same_tower = me_z == home_t
    at_home = jnp.logical_and(same_tower, me_y == home_y)

    def device(d):
        return host_of(
            lax.rem(me_z + d[0] + n_z, n_z),
            lax.rem(me_x + d[1] + n_x, n_x),
            lax.rem(me_y + d[2] + n_y, n_y),
        )

    def shift_y(y, r):
        return lax.rem(y + r + n_y, n_y)

    def goes_to_itself(r):
        return jnp.logical_and(same_tower, shift_y(me_y, r) == home_y)

    barrier = pltpu.get_barrier_semaphore()

    def greet(target):
        pl.semaphore_signal(barrier, inc=1, device_id=target, device_id_type=MESH)

    @pl.when(jnp.logical_not(at_home))
    def _():
        greet((me_z, me_x, me_y))

    targets = [device(d) for d in DIRECTIONS]
    for target in targets:
        greet(target)
    for r in range(8):

        @pl.when(jnp.logical_not(goes_to_itself(r)))
        def _():
            greet(host_of(home_t, home_x, shift_y(home_y, -r)))

    expected = len(DIRECTIONS) + 9 - at_home.astype(jnp.int32) - same_tower.astype(jnp.int32)

    row8 = lax.broadcasted_iota(jnp.int32, (8, ATOMS), 0)
    row16 = lax.broadcasted_iota(jnp.int32, (16, ATOMS), 0)
    low = row8 < 4
    comp = lax.rem(row8, 4)
    is_xyz = comp < 3
    zero8 = jnp.zeros((8, ATOMS), F32)

    for load in loads:
        load.wait()

    kinds = types_ref[...].reshape(8, ATOMS)
    table = jnp.zeros((8, ATOMS), F32)
    for kind in range(KINDS):
        table = jnp.where(kinds == kind, strength_ref[kind], table)
    lanes = lax.broadcasted_iota(jnp.int32, (1, ATOMS), 1)
    parcel[8] = zero8
    for cell in range(8):
        z, x, y = cell // 4, cell // 2 % 2, cell % 2
        live = (lanes < counts_ref[z, x, y]).astype(F32)
        for k in range(3):
            parcel[cell, pl.ds(k, 1), :] = pos_ref[k, z, x, pl.ds(y, 1), :]
            parcel[cell, pl.ds(4 + k, 1), :] = vel_ref[k, z, x, pl.ds(y, 1), :]
        parcel[cell, pl.ds(3, 1), :] = table[cell : cell + 1] * live
        seat = dest_ref[z, x, y].astype(F32)
        parcel[cell, pl.ds(7, 1), :] = jnp.full((1, ATOMS), seat, F32)
        parcel[8, pl.ds(cell, 1), pl.ds(0, 27)] = pair_ref[z, x, pl.ds(y, 1), :].astype(F32)
    delivery = pltpu.make_async_remote_copy(
        src_ref=parcel,
        dst_ref=hosted,
        send_sem=host_sem.at[0],
        recv_sem=host_sem.at[1],
        device_id=host,
        device_id_type=MESH,
    )

    def halo_copies(slot):
        copies = []
        for i, d in enumerate(DIRECTIONS):
            (sz, tz), (sx, tx), (sy, ty) = spans(d[0]), spans(d[1]), spans_y(d[2])
            copies.append(
                pltpu.make_async_remote_copy(
                    src_ref=region.at[slot, sz, sx, sy],
                    dst_ref=region.at[slot, tz, tx, ty],
                    send_sem=send_sem.at[slot, i],
                    recv_sem=recv_sem.at[slot, i],
                    device_id=targets[i],
                    device_id_type=MESH,
                )
            )
        return copies

    def constant_parts():
        for p in range(4):
            for t in range(3):
                for side in range(2):
                    half = ((0, 0), (1, 1), (0, 1))[t][side]
                    mark = jnp.where((low if half == 0 else ~low) & is_xyz, -1.0, 0.0)
                    right_ref[p, 80:96, pl.ds(256 * t + 128 * side, 128)] = jnp.concatenate(
                        [mark, mark], axis=0
                    ).astype(BF16)

    def unpack():
        for cell in range(8):
            z, x, y = cell // 4, cell // 2 % 2, cell % 2
            tile = hosted[cell]
            region[0, 1 + z, 1 + x, y] = tile[:4]
            speed[cell // 2, pl.ds(4 * y, 4), :] = jnp.where(row8[:4] < 3, tile[4:], 0.0)
            seat_ref[cell] = jnp.broadcast_to(tile[7:8], (8, ATOMS))

    def unpack_flags():
        padded = jnp.concatenate([(hosted[8] - 1.0) * 100.0] + [zero8] * 15, axis=0)
        turned = padded.T
        for cell in range(8):
            flag_ref[cell] = jnp.broadcast_to(turned[:32, cell : cell + 1], (32, ATOMS))
        for p, side in itertools.product(range(4), range(2)):
            cell, z, x = 2 * p + side, p // 2, p % 2
            rows32 = flag_ref[cell]
            for t in range(3):
                y = ((0, 0), (1, 1), (-1, 2))[t][side] - side + 1
                rows = [jnp.zeros((1, ATOMS), F32)] * 16
                for oz, ox in itertools.product(range(3), range(3)):
                    k = 9 * oz + 3 * ox + y
                    rows[4 * (z + oz) + x + ox] = rows32[k : k + 1]
                right_ref[p, 96:112, pl.ds(256 * t + 128 * side, 128)] = jnp.concatenate(
                    rows, axis=0
                ).astype(BF16)

    def shift_of(z, x, part):
        y_low, y_high = ((-1.0, 0.0), (-2.0, 1.0))[part]
        y = jnp.where(low, y_low, y_high)
        return jnp.where(
            comp == 0, z - 2.0, jnp.where(comp == 1, x - 2.0, jnp.where(comp == 2, y, 0.0))
        )

    def own_tile(slot, z, x, part):
        return jnp.concatenate(
            [region[slot, z, x, 2 * part], region[slot, z, x, 2 * part + 1]], axis=0
        )

    def strength_rows(tile):
        return jnp.concatenate(
            [
                jnp.broadcast_to(tile[3:4], (4, ATOMS)),
                jnp.broadcast_to(tile[7:8], (4, ATOMS)),
            ],
            axis=0,
        )

    def build_left(slot, z, x, part):
        column = 4 * z + x
        raw = own_tile(slot, z, x, part)
        tile = raw + shift_of(z, x, part)
        high, mid, rest = thirds(tile)
        ones = jnp.ones((24, ATOMS), F32)
        rows = [high, high, mid, mid, high, rest, ones, *thirds(tile * tile)]
        rows += [jnp.where(row16 == column, 1.0, 0.0)]
        left_ref[part, column] = jnp.concatenate(rows, axis=0).astype(BF16).T
        value = jnp.where(is_xyz, tile, 1.0) * strength_rows(raw)
        high = value.astype(BF16).astype(F32)
        value_ref[part, :, pl.ds(128 * column, 128)] = jnp.concatenate(
            [high, value - high], axis=0
        ).astype(BF16)

    def build_right(slot):
        for p in range(4):
            z, x = 1 + p // 2, 1 + p % 2
            tile = own_tile(slot, z, x, 0) + shift_of(z, x, 0)
            tile = jnp.where(is_xyz, tile, 0.0)
            terms = [2.0 * v for v in thirds(tile)]
            swapped = [swap_halves(v) for v in terms]
            squares = [-v for v in thirds(tile * tile)]
            squares[0] = jnp.where(is_xyz, squares[0], 1.0)
            for side in range(2):
                mine = low if side == 0 else ~low
                norms = [jnp.where(mine, v, 0.0) for v in squares]
                for t in range(3):
                    half = ((0, 0), (1, 1), (0, 1))[t][side]
                    keep = low if half == 0 else ~low
                    source = terms if half == side else swapped
                    high, mid, rest = [jnp.where(keep, v, 0.0) for v in source]
                    mark = jnp.where(keep & is_xyz, -1.0, 0.0)
                    rows = [high, mid, high, mid, rest, high, *norms, mark]
                    right_ref[p, 0:80, pl.ds(256 * t + 128 * side, 128)] = jnp.concatenate(
                        rows, axis=0
                    ).astype(BF16)

    def nearness(part, columns, targets):
        lhs = jnp.concatenate([left_ref[part, c] for c in columns], axis=0)
        rhs = jnp.concatenate(
            [right_ref[p, :, pl.ds(256 * t, 256)] for p, t in targets], axis=1
        )
        return jnp.dot(lhs, rhs, preferred_element_type=F32)

    def add_sums(near, part, columns, targets, first):
        near = jnp.maximum(near, 0.0)
        weight = near * near
        high = weight.astype(BF16)
        rest = (weight - high.astype(F32)).astype(BF16)
        values = jnp.concatenate(
            [value_ref[part, :, pl.ds(128 * c, 128)] for c in columns], axis=1
        )
        add = jnp.dot(values, high, preferred_element_type=F32) + jnp.dot(
            values, rest, preferred_element_type=F32
        )
        for i, (p, t) in enumerate(targets):
            more = add[:, 256 * i : 256 * i + 256]
            if first:
                total[p, t] = more
            else:
                total[p, t] += more

    def add_pairs(groups):
        parts = [
            (part, columns[at : at + CHUNK], targets, first and at == 0)
            for part, columns, targets, first in groups
            for at in range(0, len(columns), CHUNK)
        ]
        waiting = []
        for group in parts:
            waiting.append((nearness(*group[:3]), *group))
            if len(waiting) > AHEAD:
                add_sums(*waiting.pop(0))
        for group in waiting:
            add_sums(*group)

    def update(slot):
        for p in range(4):
            z, x = 1 + p // 2, 1 + p % 2
            both = total[p, 0]
            both = both[:8] + both[8:]
            other = total[p, 1]
            other = other[:8] + other[8:]
            apart = total[p, 2]
            apart = apart[:8] + apart[8:]
            sums = jnp.concatenate(
                [
                    both[:4, :128] + other[4:, :128] + apart[:4, :128],
                    both[:4, 128:] + other[4:, 128:] + apart[4:, 128:],
                ],
                axis=0,
            )
            raw = own_tile(slot, z, x, 0)
            tile = raw + shift_of(z, x, 0)
            force = -6.0 * strength_rows(raw) * (sums - tile * strength_rows(sums))
            new_speed = speed[p] + STEP_TIME * jnp.where(is_xyz, force, 0.0)
            speed[p] = new_speed
            new = raw + STEP_TIME * new_speed
            region[slot + 1, z, x, 0] = new[:4]
            region[slot + 1, z, x, 1] = new[4:]

    inner = (1, 2)
    own = [(z, x) for z in inner for x in inner]
    beside = [(z, x) for z in (0, 3) for x in inner] + [(z, x) for z in inner for x in (0, 3)]
    across = [(z, x) for z in (0, 3) for x in (0, 3)]

    def one_step(slot, carry):
        copies = halo_copies(slot)
        for copy in copies[NEAREST:FACES] + copies[:NEAREST] + copies[FACES:]:
            copy.start()
        pl.when(slot == 0)(unpack_flags)
        build_right(slot)
        for z, x in own:
            build_left(slot, z, x, 0)
        add_pairs([(0, [5, 6, 9, 10], [(p, 0), (p, 1)], True) for p in range(4)])
        for copy in copies[:NEAREST]:
            copy.wait_recv()
        for z in (0, 3):
            for x in inner:
                build_left(slot, z, x, 0)
        add_pairs(
            [
                (0, [12 * (p // 2) + 1, 12 * (p // 2) + 2], [(p, 0), (p, 1)], False)
                for p in range(4)
            ]
        )
        for copy in copies:
            copy.wait_send()
        for copy in copies[NEAREST:FACES]:
            copy.wait_recv()
        for z, x in own:
            build_left(slot, z, x, 1)
        for z in inner:
            for x in (0, 3):
                build_left(slot, z, x, 0)
        add_pairs(
            [(1, [5, 6, 9, 10], [(p, 2), (p + 1, 2)], True) for p in (0, 2)]
            + [
                (0, [4 + 3 * (p % 2), 8 + 3 * (p % 2)], [(p, 0), (p, 1)], False)
                for p in range(4)
            ]
        )
        for copy in copies[FACES:EDGES]:
            copy.wait_recv()
        for z, x in beside:
            build_left(slot, z, x, 1)
        for z, x in across:
            build_left(slot, z, x, 0)
        add_pairs(
            [(1, [12 * i + 1, 12 * i + 2], [(2 * i, 2), (2 * i + 1, 2)], False) for i in (0, 1)]
            + [(1, [4 + 3 * i, 8 + 3 * i], [(i, 2), (2 + i, 2)], False) for i in (0, 1)]
            + [
                (0, [12 * (p // 2) + 3 * (p % 2)], [(p, 0), (p, 1)], False)
                for p in range(4)
            ]
        )
        for copy in copies[EDGES:]:
            copy.wait_recv()
        for z, x in across:
            build_left(slot, z, x, 1)
        add_pairs(
            [(1, [12 * (p // 2) + 3 * (p % 2)], [(p, 2)], False) for p in range(4)]
        )
        update(slot)
        return carry

    constant_parts()
    pl.semaphore_wait(barrier, expected)

    @pl.when(jnp.logical_not(at_home))
    def _():
        delivery.start()
        delivery.wait_recv()
        delivery.wait_send()

    @pl.when(at_home)
    def _():
        hosted[...] = parcel[...]

    unpack()
    lax.fori_loop(0, STEPS, one_step, 0)

    states, moves = [], []
    for cell in range(8):
        z, x, y = cell // 4, cell // 2 % 2, cell % 2
        here = region[STEPS, 1 + z, 1 + x, y]
        moved = jnp.concatenate([here, speed[cell // 2, 4 * y : 4 * y + 4]], axis=0)
        live = jnp.broadcast_to(here[3:4], (8, ATOMS)) > 0.0
        states.append(jnp.where(live & is_xyz, moved, 0.0))
    for r in range(8):
        y = shift_y(me_y, r)
        base = (((me_z * n_x + me_x) * n_y + y) * SEATS).astype(F32)
        message = jnp.where(row8 == 3, -1.0, 0.0)
        for cell in range(8):
            seat = seat_ref[cell] - base
            hit = (seat >= 0.0) & (seat < float(SEATS))
            tagged = jnp.where(row8 == 3, seat, states[cell])
            if r == 0:
                stay_send[cell] = jnp.where(hit, tagged, jnp.where(row8 == 3, -1.0, 0.0))
            else:
                message = jnp.where(hit, tagged, message)
        if r > 0:
            send_box[r - 1] = message
        src, dst = (stay_send, stay_box) if r == 0 else (send_box.at[r - 1], box.at[r - 1])
        move = pltpu.make_async_remote_copy(
            src_ref=src,
            dst_ref=dst,
            send_sem=move_send_sem.at[r],
            recv_sem=move_recv_sem.at[r],
            device_id=(me_z, me_x, y),
            device_id_type=MESH,
        )
        moves.append(move)

        @pl.when(jnp.logical_not(goes_to_itself(r)))
        def _():
            move.start()

        @pl.when(goes_to_itself(r))
        def _():
            dst[...] = src[...]

    for r in range(8):

        @pl.when(jnp.logical_not(goes_to_itself(r)))
        def _():
            moves[r].wait_send()
            moves[r].wait_recv()

    messages = [stay_box[cell] for cell in range(8)] + [box[r] for r in range(7)]
    marks = [jnp.broadcast_to(m[3:4], (8, ATOMS)) for m in messages]
    for seat in range(SEATS):
        result = zero8
        for mark, message in zip(marks, messages):
            result = jnp.where(mark == float(seat), message, result)
        for k in range(3):
            out_pos_ref[k, pl.ds(seat, 1), :] = result[k : k + 1]
            out_vel_ref[k, pl.ds(seat, 1), :] = result[4 + k : 5 + k]


def on_device(positions, velocities, types, strength, counts, pair_list, destination):
    vmem = pl.BlockSpec(memory_space=pltpu.VMEM)
    shape = pltpu.VMEM((3, SEATS, ATOMS), F32)
    return pl.pallas_call(
        body,
        out_shape=(shape, shape),
        in_specs=[pl.BlockSpec(memory_space=pl.ANY)] * 7,
        out_specs=(vmem, vmem),
        scratch_shapes=[
            pltpu.VMEM((3, 2, 2, 2, ATOMS), F32),
            pltpu.VMEM((3, 2, 2, 2, ATOMS), F32),
            pltpu.VMEM((2, 2, 2, ATOMS), jnp.int32),
            pltpu.SMEM((KINDS,), F32),
            pltpu.SMEM((2, 2, 2), jnp.int32),
            pltpu.VMEM((2, 2, 2, 27), jnp.int32),
            pltpu.SMEM((2, 2, 2), jnp.int32),
            pltpu.SemaphoreType.DMA((7,)),
            pltpu.VMEM((STEPS + 1, 4, 4, 4, 4, ATOMS), F32),
            pltpu.VMEM((4, 8, ATOMS), F32),
            pltpu.VMEM((8, 8, ATOMS), F32),
            pltpu.VMEM((9, 8, ATOMS), F32),
            pltpu.VMEM((9, 8, ATOMS), F32),
            pltpu.VMEM((8, 32, ATOMS), F32),
            pltpu.VMEM((2, 16, ATOMS, DEPTH), BF16),
            pltpu.VMEM((4, DEPTH, 6 * ATOMS), BF16),
            pltpu.VMEM((2, 16, 16 * ATOMS), BF16),
            pltpu.VMEM((4, 3, 16, 2 * ATOMS), F32),
            pltpu.VMEM((7, 8, ATOMS), F32),
            pltpu.VMEM((8, 8, ATOMS), F32),
            pltpu.VMEM((7, 8, ATOMS), F32),
            pltpu.VMEM((8, 8, ATOMS), F32),
            pltpu.SemaphoreType.DMA((STEPS, 26)),
            pltpu.SemaphoreType.DMA((STEPS, 26)),
            pltpu.SemaphoreType.DMA((2,)),
            pltpu.SemaphoreType.DMA((8,)),
            pltpu.SemaphoreType.DMA((8,)),
        ],
        compiler_params=pltpu.CompilerParams(collective_id=0, has_side_effects=True),
    )(positions, velocities, types, strength, counts, pair_list.transpose(1, 2, 3, 0), destination)


def solution(mesh):
    return jax.shard_map(
        on_device,
        mesh=mesh,
        in_specs=(
            P(None, "tower", "px", "py", None),
            P(None, "tower", "px", "py", None),
            P("tower", "px", "py", None),
            P(),
            P("tower", "px", "py"),
            P(None, "tower", "px", "py"),
            P("tower", "px", "py"),
        ),
        out_specs=(P(None, ("tower", "px", "py"), None), P(None, ("tower", "px", "py"), None)),
        check_vma=False,
    )
```
